32 devices in a mesh: dap: 8 (over z, x), cplx: 4 (over y, core).
Axes of the slice: x: 2, y: 2, z: 4, core: 2. Of those that a mesh axis runs over, the one named last changes fastest.
Arguments:
- pair: bfloat16 [96, 384, 128], P('dap', 'cplx'), parts along dimension 1, may hold values from -6 to 6
- cotangent: bfloat16 [96, 384, 128], P('dap', 'cplx'), parts along dimension 1, may hold values from -6 to 6
- residue_mask: int32 [384], P('cplx'), parts along dimension 0, may hold values 0 or 1
- chain_ids: int32 [384], P('cplx'), parts along dimension 0, may hold values from 0 to 2, never falling along the last dimension, each value on 1 to 48 neighbouring positions
- chain_embed: float32 [2, 128], replicated, may hold values from -4 to 4
- out_norm_gain: float32 [128], replicated, may hold values from 0.25 to 1.75
- out_proj: bfloat16 [128, 512], replicated, may hold values from -0.5 to 0.5
- out_gate: bfloat16 [128, 128], replicated, may hold values from -0.5 to 0.5
- out_mid_gain: float32 [128], replicated, may hold values from 0.25 to 1.75
- out_final: bfloat16 [128, 128], replicated, may hold values from -0.5 to 0.5
- in_norm_gain: float32 [128], replicated, may hold values from 0.25 to 1.75
- in_proj: bfloat16 [128, 512], replicated, may hold values from -0.5 to 0.5
- in_gate: bfloat16 [128, 128], replicated, may hold values from -0.5 to 0.5
- in_mid_gain: float32 [128], replicated, may hold values from 0.25 to 1.75
- in_final: bfloat16 [128, 128], replicated, may hold values from -0.5 to 0.5
Outputs:
- pair_grad: bfloat16 [96, 384, 128], P('dap', 'cplx'), parts along dimension 1
- grad_proj: float32 [512, 512], P('cplx'), parts along dimension 0
- grad_gate: float32 [512, 128], P('cplx'), parts along dimension 0
- grad_final: float32 [512, 128], P('cplx'), parts along dimension 0
- grad_norm_gain: float32 [512], P('cplx'), parts along dimension 0
- grad_mid_gain: float32 [512], P('cplx'), parts along dimension 0
The draws below stay inside these ranges and needn't reach their ends.
There are 4 independent parts, one for each index of `cplx`. The reference program is written for one: setup_inputs(seed, part) draws one part's arguments, and reference() takes and returns one part's arrays. A program takes and returns all parts, laid end to end along the dimension named above; an argument that names none is the same for every part. Nothing has to cross between parts.
Inputs may be any that keep to these rules, and one draw needn't show every extreme that they name: `chain_ids`: chain numbers never fall along the residues; each chain has at most 48 residues.
All inputs are finite; a program needn't handle non-finite values.
Results may differ from the reference program's by a relative error of at most 0.019.
Values may be sent and summed in bfloat16 or wider, within the bound.
A program may use at most 128 MiB of HBM per device.

```python
import math
import jax
import jax.numpy as jnp
import numpy as np
from jax import lax

C = 128
HID = 128
N_RES = 96


def plant(result, rng, smallest, high):
    place = [jax.random.randint(jax.random.fold_in(rng, axis), (), 0, length) for axis, length in enumerate(result.shape)]
    widest = result.shape.index(max(result.shape))
    neighbour = place[:widest] + [(place[widest] + 1) % result.shape[widest]] + place[widest + 1:]
    return result.at[tuple(place)].set(smallest).at[tuple(neighbour)].set(high)


def shard_levels(key, extent, cuts, least, high):
    factor_of = 1.0
    for position, blocks in cuts:
        draws = jax.random.uniform(jax.random.fold_in(jax.random.fold_in(key, 6), position), (blocks,), jnp.float32, least / len(cuts), high / len(cuts))
        factor_of = factor_of * jnp.repeat(jnp.exp(draws), extent[position] // blocks).reshape((-1,) + (1,) * (len(extent) - 1 - position))
    return factor_of


def split_up(number_of, total, most, skew):
    loads = [(1 << 20) // math.isqrt(rank ** skew) + 1 for rank in range(2, number_of + 1)]
    surplus, counts = total - most - (number_of - 1), [1] * (number_of - 1)
    while surplus > 0:
        free = [i for i in range(number_of - 1) if counts[i] < most]
        pool, left = sum([loads[i] for i in free]), surplus
        for i in free:
            addition = min(most - counts[i], max(1, left * loads[i] // pool), surplus)
            counts[i] = counts[i] + addition
            surplus = surplus - addition
    return np.array([most] + counts)


def uneven_parts(rng, amount, total, limit, skew):
    if amount == 2:
        one = jax.random.randint(rng, (), max(1, total - limit), min(limit, total - 1) + 1)
        return jnp.stack([one, total - one])
    tallies = jnp.asarray(split_up(amount, total, limit, skew), jnp.int32)
    twos = (amount - 1) // 2
    donor, sink = tallies[1:1 + 2 * twos:2], tallies[2:2 + 2 * twos:2]
    margin = jnp.minimum(donor - 1, limit - sink)
    shifted = jax.random.randint(jax.random.fold_in(rng, 1), (twos,), 0, 1 << 20) % (margin + 1)
    tallies = tallies.at[1:1 + 2 * twos:2].set(donor - shifted).at[2:2 + 2 * twos:2].set(sink + shifted)
    return tallies[jax.random.permutation(jax.random.fold_in(rng, 2), amount)]


def normal_values(stream_key, dims, deviation, most, cuts=(), dtype=jnp.bfloat16):
    drawn = jax.random.normal(stream_key, dims, jnp.float32) * deviation
    if len(cuts) > 0:
        drawn = shard_levels(stream_key, dims, cuts, -0.22, 0.18) * drawn
    return jnp.clip(drawn, min=-most, max=most).astype(dtype)


def setup_inputs(seed: int = 0, part: int = 0) -> dict:
    arg_keys = jax.random.split(jax.random.key(seed), 16)
    part_splits = jax.random.split(jax.random.fold_in(arg_keys[15], part), 16)
    return {
        "pair": normal_values(part_splits[0], (N_RES, N_RES, C), 1.0, 6.0, ((0, 8),)),
        "cotangent": normal_values(part_splits[1], (N_RES, N_RES, C), 1.0, 6.0, ((0, 8),)),
        "residue_mask": plant((jax.random.randint(part_splits[2], (N_RES,), 0, 8) < 7).astype(jnp.int32), jax.random.fold_in(part_splits[2], 1), 0, 1),
        "chain_ids": jnp.searchsorted(jnp.cumsum(uneven_parts(part_splits[3], 3, N_RES, N_RES // 2, 0)), jnp.arange(N_RES), side="right").astype(jnp.int32),
        "chain_embed": normal_values(arg_keys[4], (2, C), 1.0, 4.0, (), jnp.float32),
        "out_norm_gain": jnp.clip(1.0 + 0.15 * jax.random.normal(arg_keys[5], (C,), jnp.float32), 0.25, 1.75),
        "out_proj": normal_values(arg_keys[6], (C, 4 * HID), C ** -0.5, 0.5),
        "out_gate": normal_values(arg_keys[7], (C, C), C ** -0.5, 0.5),
        "out_mid_gain": jnp.clip(1.0 + 0.15 * jax.random.normal(arg_keys[8], (HID,), jnp.float32), 0.25, 1.75),
        "out_final": normal_values(arg_keys[9], (HID, C), HID ** -0.5, 0.5),
        "in_norm_gain": jnp.clip(1.0 + 0.15 * jax.random.normal(arg_keys[10], (C,), jnp.float32), 0.25, 1.75),
        "in_proj": normal_values(arg_keys[11], (C, 4 * HID), C ** -0.5, 0.5),
        "in_gate": normal_values(arg_keys[12], (C, C), C ** -0.5, 0.5),
        "in_mid_gain": jnp.clip(1.0 + 0.15 * jax.random.normal(arg_keys[13], (HID,), jnp.float32), 0.25, 1.75),
        "in_final": normal_values(arg_keys[14], (HID, C), HID ** -0.5, 0.5),
    }


def layer_norm(values_in, gain):
    average = lax.optimization_barrier(jnp.mean(values_in, axis=-1, keepdims=True))
    centred = values_in - average
    variance = lax.optimization_barrier(jnp.mean(centred * centred, axis=-1, keepdims=True))
    return centred * jax.lax.rsqrt(variance + 1e-05) * gain

def gated_pair(projected, pair_mask, hidden_width):
    masked = pair_mask[..., None]
    left_act = masked * jax.nn.sigmoid(projected[..., :hidden_width]) * projected[..., hidden_width:2 * hidden_width]
    right_act = masked * jax.nn.sigmoid(projected[..., 2 * hidden_width:3 * hidden_width]) * projected[..., 3 * hidden_width:]
    return (left_act, right_act)

def reference(pair, cotangent, residue_mask, chain_ids, chain_embed, out_norm_gain, out_proj, out_gate, out_mid_gain, out_final, in_norm_gain, in_proj, in_gate, in_mid_gain, in_final):
    f32 = jnp.float32
    bf16 = jnp.bfloat16
    hidden_width = out_final.shape[0]
    res_count = pair.shape[0]
    inv_count = 1.0 / res_count
    pair_mask = (residue_mask[:, None] * residue_mask[None, :]).astype(f32)
    same_chain = chain_ids[:, None] == chain_ids[None, :]
    start = pair.astype(f32) + jnp.where(same_chain[..., None], chain_embed[1], chain_embed[0])
    out_normed = layer_norm(start, out_norm_gain).astype(bf16)
    projected = jnp.dot(out_normed, out_proj, preferred_element_type=f32)
    left_act, right_act = gated_pair(projected, pair_mask, hidden_width)
    left_b = left_act.astype(bf16)
    right_b = right_act.astype(bf16)
    x_out = jnp.einsum('ikc,jkc->ijc', left_b.astype(f32), right_b.astype(f32))
    y_out = layer_norm(x_out, out_mid_gain).astype(bf16)
    update = jax.nn.sigmoid(jnp.dot(out_normed, out_gate, preferred_element_type=f32)) * jnp.dot(y_out, out_final, preferred_element_type=f32)
    pair_mid = (start + update).astype(bf16)
    mid_f32 = pair_mid.astype(f32)
    normed_f32, norm_back = jax.vjp(layer_norm, mid_f32, in_norm_gain)
    in_normed = normed_f32.astype(bf16)
    proj_in = jnp.dot(in_normed, in_proj, preferred_element_type=f32)
    (left_in, right_in), glu_back = jax.vjp(lambda proj_val: gated_pair(proj_val, pair_mask, hidden_width), proj_in)
    left_ib = left_in.astype(bf16)
    right_ib = right_in.astype(bf16)
    x_in = jnp.einsum('kic,kjc->ijc', left_ib.astype(f32), right_ib.astype(f32))
    y_f32, mid_back = jax.vjp(layer_norm, x_in, in_mid_gain)
    y_in = y_f32.astype(bf16)
    logit = jnp.dot(in_normed, in_gate, preferred_element_type=f32)
    value = jnp.dot(y_in, in_final, preferred_element_type=f32)
    sigma = jax.nn.sigmoid(logit)
    upstream = cotangent.astype(f32)
    grad_value = (upstream * sigma).astype(bf16)
    grad_logit = (upstream * value * sigma * (1.0 - sigma)).astype(bf16)
    grad_final = jnp.einsum('ijc,ijd->cd', y_in.astype(f32), grad_value.astype(f32)) * inv_count
    grad_gate = jnp.einsum('ijc,ijd->cd', in_normed.astype(f32), grad_logit.astype(f32)) * inv_count
    grad_y = jnp.dot(grad_value, in_final.T, preferred_element_type=f32)
    grad_x, grad_mid = mid_back(grad_y)
    grad_x_b = grad_x.astype(bf16).astype(f32)
    grad_a = jnp.einsum('kjc,ijc->kic', right_ib.astype(f32), grad_x_b)
    grad_b = jnp.einsum('kic,ijc->kjc', left_ib.astype(f32), grad_x_b)
    grad_p = glu_back((grad_a, grad_b))[0].astype(bf16)
    grad_proj = jnp.einsum('ijc,ijd->cd', in_normed.astype(f32), grad_p.astype(f32)) * inv_count
    grad_normed = jnp.dot(grad_p, in_proj.T, preferred_element_type=f32) + jnp.dot(grad_logit, in_gate.T, preferred_element_type=f32)
    grad_z, grad_norm = norm_back(grad_normed)
    pair_grad = (upstream + grad_z).astype(bf16)
    return (pair_grad, grad_proj, grad_gate, grad_final, grad_norm * inv_count, grad_mid * inv_count)
```

```python
import functools

import jax
import jax.numpy as jnp
from jax import lax
from jax.experimental import pallas as pl
from jax.experimental.pallas import tpu as pltpu
from jax.sharding import PartitionSpec as P

F32 = jnp.float32
BF16 = jnp.bfloat16
LANES = 128
A_OUT, B_OUT, X_OUT, A_IN, B_IN, X_IN, G_X, G_A, G_B, P_SUM, P_ALL, H_SUM, H_ALL, GAINS = range(14)


def tn(w, x):
    return lax.dot_general(w, x, (((0,), (0,)), ((), ())), preferred_element_type=F32)


def nn(w, x):
    return jnp.dot(w, x, preferred_element_type=F32)


def nt(w, x):
    return lax.dot_general(w, x, (((1,), (1,)), ((), ())), preferred_element_type=F32)


def sigmoid(v):
    return 1.0 / (1.0 + jnp.exp(-v))


def norm_stats(v):
    centred = v - jnp.mean(v, axis=0, keepdims=True)
    inv = lax.rsqrt(jnp.mean(centred * centred, axis=0, keepdims=True) + 1e-05)
    return centred * inv, inv


def norm_back(grad, hat, inv, gain):
    scaled = grad * gain
    m1 = jnp.mean(scaled, axis=0, keepdims=True)
    m2 = jnp.mean(scaled * hat, axis=0, keepdims=True)
    return inv * (scaled - m1 - hat * m2)


def lane_sum(v):
    return jnp.sum(v, axis=1, keepdims=True)


def kernel(
    n, rows, res, lc,
    pair, cot, residues, chains, embed, gain_on, gain_om, gain_in, gain_im, out_proj, out_gate, out_final, in_proj, in_gate, in_final,
    grad_out, gp_out, gg_out, gf_out, gn_out, gm_out,
    cols, masks, in_q, start, normed, gate, in_p, cot_t, mid, logit_s, gv, gy, gl,
    a_s, b_s, x_s, a_r, b_r, x_r,
    a2_s, b2_s, x2_s, a2_r, b2_r, x2_r,
    gx_s, gx_r, ga_s, gb_s, ga_r, gb_r,
    slab_a, slab_b, slab_o, slab_p, mat_a, mat_b, mat_x,
    acc_p, acc_g, acc_f, acc_n, acc_m, g_s, g_r, t_s, t_r, h_s, h_r, u_s, u_r, w_s, w_r,
    send_sem, recv_sem,
):
    me = lax.axis_index("dap")
    c = start.shape[0]
    per = c // n
    total = rows * res
    chunks = total // lc
    crows = lc // res
    tiles = -(-res // LANES)
    inv_count = 1.0 / res

    barrier = pltpu.get_barrier_semaphore()
    for p in range(1, n):
        pl.semaphore_signal(
            barrier, inc=1, device_id={"dap": lax.rem(me + p, n)},
            device_id_type=pl.DeviceIdType.MESH,
        )

    def copy_to(sem, src, dst, peer):
        return pltpu.make_async_remote_copy(
            src_ref=src, dst_ref=dst, send_sem=send_sem.at[sem], recv_sem=recv_sem.at[sem],
            device_id={"dap": peer}, device_id_type=pl.DeviceIdType.MESH,
        )

    def spread(which, src, dst, k=0, ds=None):
        def view(ref, at):
            return ref.at[at] if ds is None else ref.at[at, :, ds]

        for p in range(1, n):
            peer = lax.rem(me + p, n)
            copy_to(which * chunks + k, view(src, peer), view(dst, me), peer).start()
        if ds is None:
            dst[me] = src[me]
        else:
            dst[me, :, ds] = src[me, :, ds]

    def collect(which, src, dst, k=0, ds=None):
        def view(ref):
            return ref.at[pl.ds(0, n - 1)] if ds is None else ref.at[pl.ds(0, n - 1), :, ds]

        copy_to(which * chunks + k, view(src), view(dst), lax.rem(me + 1, n)).wait()

    def lanes_of(k):
        return pl.ds(pl.multiple_of(k * lc, lc), lc)

    def put(ref, ds, value):
        ref[:, :, ds] = value.reshape(n, per, lc).astype(BF16)

    def take(ref, ds):
        return ref[:, :, ds].astype(F32).reshape(c, lc)

    def to_slab(ref, slab, k, by_chunk=False):
        for s in range(n):
            block = ref[s, :, lanes_of(k)].astype(F32)
            row = (k * n + s) * crows if by_chunk else s * rows + k * crows
            for i in range(crows):
                part = block[:, i * res : (i + 1) * res]
                at = pl.ds(pl.multiple_of((row + i) * per, per), per)
                for t in range(tiles):
                    width = min(LANES, res - t * LANES)
                    slab[t, at, :width] = part[:, t * LANES : t * LANES + width]

    def matrix(slab, ch, first=0, count=res):
        at = pl.ds(first * per + ch, count, stride=per)
        parts = [slab[t, at, :] for t in range(tiles)]
        whole = parts[0] if tiles == 1 else jnp.concatenate(parts, axis=1)
        return whole[:, :res].astype(BF16)

    def keep(slab, ch, value, first=0):
        count = value.shape[0]
        pad = tiles * LANES - res
        if pad:
            value = jnp.concatenate([value, jnp.zeros((count, pad), F32)], axis=1)
        for t in range(tiles):
            at = pl.ds(first * per + ch, count, stride=per)
            slab[t, at, :] = value[:, t * LANES : (t + 1) * LANES]

    def from_slab(slab, ref, k, by_chunk=False):
        for s in range(n):
            row = (k * n + s) * crows if by_chunk else s * rows + k * crows
            parts = []
            for i in range(crows):
                at = pl.ds(pl.multiple_of((row + i) * per, per), per)
                for t in range(tiles):
                    width = min(LANES, res - t * LANES)
                    parts.append(slab[t, at, :width])
            ref[s, :, lanes_of(k)] = jnp.concatenate(parts, axis=1).astype(BF16)

    def early():
        return jnp.concatenate([acc_g[...], acc_f[...]], axis=1) * inv_count

    def hand_round(which, src, mine, dst):
        summed = jnp.sum(src[...].astype(F32), axis=0).astype(BF16)
        mine[...] = summed
        for p in range(1, n):
            copy_to(which * chunks, mine, dst.at[me], lax.rem(me + p, n)).start()
        dst[me] = summed

    def gathered(which, dst):
        block = dst.at[pl.ds(0, n - 1)]
        copy_to(which * chunks, block, block, lax.rem(me + 1, n)).wait()
        return dst[...].astype(F32).reshape(c, dst.shape[2])

    params = [embed[...], gain_on[...], gain_om[...], gain_in[...], gain_im[...]]
    cols[...] = jnp.concatenate(params + [jnp.zeros((2, c), F32)], axis=0).T
    here = lax.broadcasted_iota(jnp.int32, (rows, res), 1) == (
        lax.broadcasted_iota(jnp.int32, (rows, res), 0) + me * rows
    )
    row_mask = jnp.sum(jnp.where(here, residues[...], 0).astype(F32), axis=1, keepdims=True)
    row_chain = jnp.sum(jnp.where(here, chains[...], 0).astype(F32), axis=1, keepdims=True)
    both = row_mask * residues[...].astype(F32)
    same_chain = jnp.where(row_chain == chains[...].astype(F32), 1.0, 0.0)
    masks[0:1, :] = jnp.concatenate([both[i : i + 1] for i in range(rows)], axis=1)
    masks[1:2, :] = jnp.concatenate([same_chain[i : i + 1] for i in range(rows)], axis=1)
    emb0, emb1 = cols[:, 0:1], cols[:, 1:2]
    g_on, g_om, g_in, g_im = (cols[:, q : q + 1] for q in range(2, 6))

    def project(k):
        ds = lanes_of(k)
        same = masks[1:2, ds] > 0.5
        x = pair[ds, :].astype(F32).T + jnp.where(same, emb1, emb0)
        start[:, ds] = x
        hat, _ = norm_stats(x)
        nb = (hat * g_on).astype(BF16)
        normed[:, ds] = nb
        p = tn(out_proj[...], nb)
        pm = masks[0:1, ds]
        put(a_s, ds, pm * sigmoid(p[:c]) * p[c : 2 * c])
        put(b_s, ds, pm * sigmoid(p[2 * c : 3 * c]) * p[3 * c :])

    project(0)
    pl.semaphore_wait(barrier, n - 1)
    spread(B_OUT, b_s, b_r, 0, lanes_of(0))

    @pl.loop(1, chunks)
    def _(k):
        project(k)
        spread(B_OUT, b_s, b_r, k, lanes_of(k))

    @pl.loop(0, chunks)
    def _(k):
        spread(A_OUT, a_s, a_r, k, lanes_of(k))

    @pl.loop(0, chunks)
    def _(k):
        ds = lanes_of(k)
        gate[:, ds] = sigmoid(tn(out_gate[...], normed[:, ds]))
        cot_t[:, ds] = cot[ds, :].astype(F32).T

    @pl.loop(0, chunks)
    def _(k):
        collect(B_OUT, b_s, b_r, k, lanes_of(k))
        to_slab(b_r, slab_b, k)

    for ch in range(per):
        mat_b[ch] = matrix(slab_b, ch)

    group = n * crows

    @pl.loop(0, chunks)
    def _(k):
        ds = lanes_of(k)
        collect(A_OUT, a_s, a_r, k, ds)
        to_slab(a_r, slab_a, k, True)
        for ch in range(per):
            keep(slab_o, ch, nt(matrix(slab_a, ch, k * group, group), mat_b[ch]), k * group)
        from_slab(slab_o, x_s, k, True)
        spread(X_OUT, x_s, x_r, k, ds)

    @pl.loop(0, chunks)
    def _(k):
        ds = lanes_of(k)
        collect(X_OUT, x_s, x_r, k, ds)
        hat, _ = norm_stats(take(x_r, ds))
        y = (hat * g_om).astype(BF16)
        m = (start[:, ds] + gate[:, ds] * tn(out_final[...], y)).astype(BF16)
        mid[:, ds] = m
        hat, _ = norm_stats(m.astype(F32))
        nb = (hat * g_in).astype(BF16)
        normed[:, ds] = nb
        p = tn(in_proj[...], nb)
        in_p[:, ds] = p
        pm = masks[0:1, ds]
        put(a2_s, ds, pm * sigmoid(p[:c]) * p[c : 2 * c])
        put(b2_s, ds, pm * sigmoid(p[2 * c : 3 * c]) * p[3 * c :])
        spread(A_IN, a2_s, a2_r, k, ds)
        spread(B_IN, b2_s, b2_r, k, ds)

    @pl.loop(0, chunks)
    def _(k):
        ds = lanes_of(k)
        s = sigmoid(tn(in_gate[...], normed[:, ds]))
        logit_s[:, ds] = s
        v = (cot_t[:, ds] * s).astype(BF16)
        gv[:, ds] = v
        gy[:, ds] = nn(in_final[...], v)

    acc_p[...] = jnp.zeros_like(acc_p)
    acc_g[...] = jnp.zeros_like(acc_g)
    acc_f[...] = jnp.zeros_like(acc_f)
    acc_n[...] = jnp.zeros_like(acc_n)
    acc_m[...] = jnp.zeros_like(acc_m)

    @pl.loop(0, chunks)
    def _(k):
        collect(A_IN, a2_s, a2_r, k, lanes_of(k))
        to_slab(a2_r, slab_a, k)
        collect(B_IN, b2_s, b2_r, k, lanes_of(k))
        to_slab(b2_r, slab_b, k)

    for ch in range(per):
        a = matrix(slab_a, ch)
        b = matrix(slab_b, ch)
        mat_a[ch] = a
        mat_b[ch] = b
        keep(slab_o, ch, tn(a, b))

    @pl.loop(0, chunks)
    def _(k):
        from_slab(slab_o, x2_s, k)
        spread(X_IN, x2_s, x2_r, k, lanes_of(k))

    @pl.loop(0, chunks)
    def _(k):
        ds = lanes_of(k)
        collect(X_IN, x2_s, x2_r, k, ds)
        hat, inv = norm_stats(take(x2_r, ds))
        y = (hat * g_im).astype(BF16)
        value = tn(in_final[...], y)
        s = logit_s[:, ds]
        grad_l = (cot_t[:, ds] * value * s * (1.0 - s)).astype(BF16)
        gl[:, ds] = grad_l
        g = gy[:, ds]
        acc_m[...] += lane_sum(g * hat)
        put(gx_s, ds, norm_back(g, hat, inv, g_im))
        spread(G_X, gx_s, gx_r, k, ds)
        acc_f[...] += nt(y, gv[:, ds])

    @pl.loop(0, chunks)
    def _(k):
        ds = lanes_of(k)
        grad_l = gl[:, ds]
        acc_g[...] += nt(normed[:, ds], grad_l)
        gy[:, ds] = nn(in_gate[...], grad_l)

    h_s[...] = early().reshape(n, per, 2 * c).astype(BF16)
    spread(H_SUM, h_s, h_r)

    @pl.loop(0, chunks)
    def _(k):
        collect(G_X, gx_s, gx_r, k, lanes_of(k))
        to_slab(gx_r, slab_a, k)

    for ch in range(per):
        gx = matrix(slab_a, ch)
        mat_x[ch] = gx
        keep(slab_o, ch, nt(mat_b[ch], gx))

    @pl.loop(0, chunks)
    def _(k):
        from_slab(slab_o, ga_s, k)
        spread(G_A, ga_s, ga_r, k, lanes_of(k))

    for ch in range(per):
        keep(slab_p, ch, nn(mat_a[ch], mat_x[ch]))

    @pl.loop(0, chunks)
    def _(k):
        from_slab(slab_p, gb_s, k)
        spread(G_B, gb_s, gb_r, k, lanes_of(k))

    collect(H_SUM, h_s, h_r)
    hand_round(H_ALL, h_r, u_s, u_r)

    @pl.loop(0, chunks)
    def _(k):
        ds = lanes_of(k)
        collect(G_A, ga_s, ga_r, k, ds)
        collect(G_B, gb_s, gb_r, k, ds)
        pm = masks[0:1, ds]
        s0 = sigmoid(in_p[:c, ds])
        s2 = sigmoid(in_p[2 * c : 3 * c, ds])
        ga = take(ga_r, ds) * pm * s0
        gb = take(gb_r, ds) * pm * s2
        q0 = (ga * in_p[c : 2 * c, ds] * (1.0 - s0)).astype(BF16)
        q2 = (gb * in_p[3 * c :, ds] * (1.0 - s2)).astype(BF16)
        q = jnp.concatenate([q0, ga.astype(BF16), q2, gb.astype(BF16)], axis=0)
        in_q[:, ds] = q
        acc_p[...] += nt(normed[:, ds], q)

    g_s[...] = (acc_p[...] * inv_count).reshape(n, per, 4 * c).astype(BF16)
    spread(P_SUM, g_s, g_r)

    @pl.loop(0, chunks)
    def _(k):
        ds = lanes_of(k)
        g = nn(in_proj[...], in_q[:, ds]) + gy[:, ds]
        hat, inv = norm_stats(mid[:, ds].astype(F32))
        acc_n[...] += lane_sum(g * hat)
        z = cot_t[:, ds] + norm_back(g, hat, inv, g_in)
        grad_out[ds, :] = z.T.astype(BF16)

    lane = lax.broadcasted_iota(jnp.int32, (c, LANES), 1)
    gains = jnp.where(lane == 0, acc_n[...], jnp.where(lane == 1, acc_m[...], 0.0))
    w_s[...] = (gains * inv_count).T[:8]
    for p in range(1, n):
        copy_to(GAINS * chunks, w_s, w_r.at[me], lax.rem(me + p, n)).start()
    w_r[me] = w_s[...]
    collect(P_SUM, g_s, g_r)
    hand_round(P_ALL, g_r, t_s, t_r)
    both = gathered(H_ALL, u_r)
    gg_out[...] = both[:, :c]
    gf_out[...] = both[:, c:]
    block = w_r.at[pl.ds(0, n - 1)]
    copy_to(GAINS * chunks, block, block, lax.rem(me + 1, n)).wait()
    gain_sums = jnp.sum(w_r[...], axis=0)
    gn_out[...] = gain_sums[0:1]
    gm_out[...] = gain_sums[1:2]
    gp_out[...] = gathered(P_ALL, t_r)


def write_out(*refs):
    sems = refs[-1]
    copies = [pltpu.make_async_copy(refs[q], refs[q + 6], sems.at[q]) for q in range(6)]
    for copy in copies:
        copy.start()
    for copy in copies:
        copy.wait()


def shards(n, pair, cotangent, residue_mask, chain_ids, chain_embed, out_norm_gain, out_proj,
           out_gate, out_mid_gain, out_final, in_norm_gain, in_proj, in_gate, in_mid_gain, in_final):
    rows, res, c = pair.shape
    total = rows * res
    per = c // n
    lc = res * min(
        q for q in range(1, rows + 1)
        if rows % q == 0 and q * res % LANES == 0 and (rows // q <= 3)
    )
    tiles = -(-res // LANES)
    def full(dtype):
        return pltpu.VMEM((c, total), dtype)

    swap = pltpu.VMEM((n, per, total), BF16)
    slab = pltpu.VMEM((tiles, res * per, LANES), F32)
    mats = pltpu.VMEM((per, res, res), BF16)
    wide = 4 * c
    scratch = [
        pltpu.VMEM((c, 8), F32), pltpu.VMEM((2, total), F32), pltpu.VMEM((4 * c, total), BF16), full(F32), full(BF16), full(F32),
        pltpu.VMEM((4 * c, total), F32), full(F32), full(BF16), full(F32), full(BF16), full(F32),
        full(BF16),
    ] + [swap] * 18 + [slab] * 4 + [mats] * 3 + [
        pltpu.VMEM((c, 4 * c), F32), pltpu.VMEM((c, c), F32), pltpu.VMEM((c, c), F32),
        pltpu.VMEM((c, 1), F32), pltpu.VMEM((c, 1), F32),
        pltpu.VMEM((n, per, wide), BF16), pltpu.VMEM((n, per, wide), BF16),
        pltpu.VMEM((per, wide), BF16), pltpu.VMEM((n, per, wide), BF16),
        pltpu.VMEM((n, per, 2 * c), BF16), pltpu.VMEM((n, per, 2 * c), BF16),
        pltpu.VMEM((per, 2 * c), BF16), pltpu.VMEM((n, per, 2 * c), BF16),
        pltpu.VMEM((8, c), F32), pltpu.VMEM((n, 8, c), F32),
        pltpu.SemaphoreType.DMA((14 * (total // lc),)), pltpu.SemaphoreType.DMA((14 * (total // lc),)),
    ]
    vmem = pl.BlockSpec(memory_space=pltpu.VMEM)
    results = pl.pallas_call(
        functools.partial(kernel, n, rows, res, lc),
        out_shape=(
            pltpu.VMEM((total, c), BF16),
            pltpu.VMEM((c, 4 * c), F32),
            pltpu.VMEM((c, c), F32),
            pltpu.VMEM((c, c), F32),
            pltpu.VMEM((1, c), F32),
            pltpu.VMEM((1, c), F32),
        ),
        in_specs=[vmem] * 15,
        out_specs=(vmem,) * 6,
        scratch_shapes=scratch,
        compiler_params=pltpu.CompilerParams(
            collective_id=0, has_side_effects=True, vmem_limit_bytes=56 * 1024 * 1024
        ),
    )(
        pair.reshape(total, c), cotangent.reshape(total, c),
        residue_mask.reshape(1, res), chain_ids.reshape(1, res), chain_embed,
        out_norm_gain.reshape(1, c), out_mid_gain.reshape(1, c),
        in_norm_gain.reshape(1, c), in_mid_gain.reshape(1, c),
        out_proj, out_gate, out_final, in_proj, in_gate, in_final,
    )
    shapes = [((total, c), BF16), ((c, 4 * c), F32), ((c, c), F32), ((c, c), F32), ((1, c), F32), ((1, c), F32)]
    grad, gp, gg, gf, gn, gm = pl.pallas_call(
        write_out,
        out_shape=[jax.ShapeDtypeStruct(*shape) for shape in shapes],
        in_specs=[pl.BlockSpec(memory_space=pltpu.VMEM)] * 6,
        out_specs=[pl.BlockSpec(memory_space=pl.ANY)] * 6,
        scratch_shapes=[pltpu.SemaphoreType.DMA((6,))],
    )(*[pltpu.with_memory_space_constraint(r, pltpu.VMEM) for r in results])
    return grad.reshape(rows, res, c), gp, gg, gf, gn.reshape(c), gm.reshape(c)


def solution(mesh):
    split = P("dap", "cplx", None)
    return jax.shard_map(
        functools.partial(shards, mesh.shape["dap"]),
        mesh=mesh,
        in_specs=(split, split, P("cplx"), P("cplx")) + (P(),) * 11,
        out_specs=(split, P("cplx", None), P("cplx", None), P("cplx", None), P("cplx"), P("cplx")),
        check_vma=False,
    )
```

```python
import functools

import jax
import jax.numpy as jnp
from jax import lax
from jax.experimental import pallas as pl
from jax.experimental.pallas import tpu as pltpu
from jax.sharding import PartitionSpec as P

F32 = jnp.float32
BF16 = jnp.bfloat16
LANES = 128
PAD = 8
A_OUT, B_OUT, X_OUT, A_IN, B_IN, X_IN, G_X, G_A, G_B, P_SUM, P_ALL, H_SUM, H_ALL, GAINS = range(14)


def tn(w, x):
    return lax.dot_general(w, x, (((0,), (0,)), ((), ())), preferred_element_type=F32)


def nn(w, x):
    return jnp.dot(w, x, preferred_element_type=F32)


def nt(w, x):
    return lax.dot_general(w, x, (((1,), (1,)), ((), ())), preferred_element_type=F32)


def sigmoid(v):
    return 1.0 / (1.0 + jnp.exp(-v))


def norm_stats(v):
    centred = v - jnp.mean(v, axis=0, keepdims=True)
    inv = lax.rsqrt(jnp.mean(centred * centred, axis=0, keepdims=True) + 1e-05)
    return centred * inv, inv


def norm_back(grad, hat, inv, gain):
    scaled = grad * gain
    m1 = jnp.mean(scaled, axis=0, keepdims=True)
    m2 = jnp.mean(scaled * hat, axis=0, keepdims=True)
    return inv * (scaled - m1 - hat * m2)


def lane_sum(v):
    return jnp.sum(v, axis=1, keepdims=True)


def kernel(
    n, rows, res, lc, pitch,
    pair, cot, residues, chains, embed, gain_on, gain_om, gain_in, gain_im, out_proj, out_gate, out_final, in_proj, in_gate, in_final,
    grad_out, gp_out, gg_out, gf_out, gn_out, gm_out,
    cols, masks, in_q, start, normed, gate, in_p, cot_t, mid, logit_s, gv, gy, gl,
    a_s, b_s, x_s, a_r, b_r, x_r,
    a2_s, b2_s, x2_s, a2_r, b2_r, x2_r,
    gx_s, gx_r, ga_s, gb_s, ga_r, gb_r,
    slab_a, slab_b, slab_o, mat_a, mat_b,
    acc_p, acc_g, acc_f, acc_n, acc_m, g_s, g_r, t_s, t_r, h_s, h_r, u_s, u_r, w_s, w_r,
    send_sem, recv_sem,
):
    me = lax.axis_index("dap")
    c = start.shape[0]
    per = c // n
    m = n // 2
    parts, hs = a_s.shape[1], a_s.shape[2]
    mine = lax.rem(me, m)
    base = me - mine
    away = m - base
    half = m * rows
    total = rows * res
    chunks = total // lc
    crows = lc // res
    tiles = -(-res // LANES)
    inv_count = 1.0 / res

    barrier = pltpu.get_barrier_semaphore()
    for p in range(1, n):
        pl.semaphore_signal(
            barrier, inc=1, device_id={"dap": lax.rem(me + p, n)},
            device_id_type=pl.DeviceIdType.MESH,
        )

    def copy_to(sem, src, dst, peer):
        return pltpu.make_async_remote_copy(
            src_ref=src, dst_ref=dst, send_sem=send_sem.at[sem], recv_sem=recv_sem.at[sem],
            device_id={"dap": peer}, device_id_type=pl.DeviceIdType.MESH,
        )

    def flag(which, k=0, h=0):
        return (which * parts + h) * chunks + k

    def near(which, src, dst, h, k):
        ds = lanes_of(k)
        for p in range(1, m):
            slot = lax.rem(mine + p, m)
            copy_to(flag(which, k, h), src.at[slot, h, :, ds], dst.at[mine, h, :, ds], base + slot).start()
        dst[mine, h, :, ds] = src[mine, h, :, ds]

    def far(which, src, dst, h, k, by_peer=False):
        ds = lanes_of(k)
        for p in range(m):
            slot = lax.rem(mine + p, m)
            peer = away + slot
            copy_to(flag(which, k, h), src.at[peer if by_peer else slot, h, :, ds], dst.at[me, h, :, ds], peer).start()
        for p in range(1, m):
            slot = lax.rem(mine + p, m)
            peer = base + slot
            copy_to(flag(which, k, h), src.at[peer if by_peer else slot, h, :, ds], dst.at[me, h, :, ds], peer).start()
        dst[me, h, :, ds] = src[me if by_peer else mine, h, :, ds]

    def collect(which, dst, h, k):
        block = dst.at[pl.ds(0, dst.shape[0] - 1), h, :, lanes_of(k)]
        copy_to(flag(which, k, h), block, block, lax.rem(me + 1, n)).wait()

    def spread(which, src, dst):
        for p in range(1, n):
            peer = lax.rem(me + p, n)
            copy_to(flag(which), src.at[peer], dst.at[me], peer).start()
        dst[me] = src[me]

    def gather(which, dst):
        block = dst.at[pl.ds(0, n - 1)]
        copy_to(flag(which), block, block, lax.rem(me + 1, n)).wait()

    def lanes_of(k):
        return pl.ds(pl.multiple_of(k * lc, lc), lc)

    def put(ref, ds, value):
        ref[:, :, :, ds] = value.reshape(m, parts, hs, lc).astype(BF16)

    def take(ref, ds):
        return ref[:, :, :, ds].astype(F32).reshape(c, lc)

    def take_sum(ref, ds):
        both = ref[pl.ds(0, m), :, :, ds].astype(F32) + ref[pl.ds(m, m), :, :, ds].astype(F32)
        return both.reshape(c, lc)

    def to_slab(ref, slab, h, k):
        for s in range(ref.shape[0]):
            block = ref[s, h, :, lanes_of(k)].astype(F32)
            row = s * rows + k * crows
            for i in range(crows):
                part = block[:, i * res : (i + 1) * res]
                at = pl.ds(pl.multiple_of((row + i) * pitch + h * hs, 8), hs)
                for t in range(tiles):
                    width = min(LANES, res - t * LANES)
                    slab[t, at, :width] = part[:, t * LANES : t * LANES + width]

    def matrix(slab, ch, count):
        at = pl.ds(ch, count, stride=pitch)
        pieces = [slab[t, at, :] for t in range(tiles)]
        whole = pieces[0] if tiles == 1 else jnp.concatenate(pieces, axis=1)
        return whole[:, :res].astype(BF16)

    def keep(slab, ch, value):
        count = value.shape[0]
        pad = tiles * LANES - res
        if pad:
            value = jnp.concatenate([value, jnp.zeros((count, pad), F32)], axis=1)
        for t in range(tiles):
            slab[t, pl.ds(ch, count, stride=pitch), :] = value[:, t * LANES : (t + 1) * LANES]

    def from_slab(slab, ref, h, k):
        for s in range(ref.shape[0]):
            row = s * rows + k * crows
            pieces = []
            for i in range(crows):
                at = pl.ds(pl.multiple_of((row + i) * pitch + h * hs, 8), hs)
                for t in range(tiles):
                    width = min(LANES, res - t * LANES)
                    pieces.append(slab[t, at, :width])
            ref[s, h, :, lanes_of(k)] = jnp.concatenate(pieces, axis=1).astype(BF16)

    def early():
        return jnp.concatenate([acc_g[...], acc_f[...]], axis=1) * inv_count

    def hand_round(which, src, own, dst):
        summed = jnp.sum(src[...].astype(F32), axis=0).astype(BF16)
        own[...] = summed
        for p in range(1, n):
            copy_to(flag(which), own, dst.at[me], lax.rem(me + p, n)).start()
        dst[me] = summed

    def gathered(which, dst):
        gather(which, dst)
        return dst[...].astype(F32).reshape(c, dst.shape[2])

    params = [embed[...], gain_on[...], gain_om[...], gain_in[...], gain_im[...]]
    cols[...] = jnp.concatenate(params + [jnp.zeros((2, c), F32)], axis=0).T
    here = lax.broadcasted_iota(jnp.int32, (rows, res), 1) == (
        lax.broadcasted_iota(jnp.int32, (rows, res), 0) + me * rows
    )
    row_mask = jnp.sum(jnp.where(here, residues[...], 0).astype(F32), axis=1, keepdims=True)
    row_chain = jnp.sum(jnp.where(here, chains[...], 0).astype(F32), axis=1, keepdims=True)
    both = row_mask * residues[...].astype(F32)
    same_chain = jnp.where(row_chain == chains[...].astype(F32), 1.0, 0.0)
    masks[0:1, :] = jnp.concatenate([both[i : i + 1] for i in range(rows)], axis=1)
    masks[1:2, :] = jnp.concatenate([same_chain[i : i + 1] for i in range(rows)], axis=1)
    emb0, emb1 = cols[:, 0:1], cols[:, 1:2]
    g_on, g_om, g_in, g_im = (cols[:, q : q + 1] for q in range(2, 6))

    def project(k):
        ds = lanes_of(k)
        same = masks[1:2, ds] > 0.5
        x = pair[ds, :].astype(F32).T + jnp.where(same, emb1, emb0)
        start[:, ds] = x
        hat, _ = norm_stats(x)
        nb = (hat * g_on).astype(BF16)
        normed[:, ds] = nb
        p = tn(out_proj[...], nb)
        pm = masks[0:1, ds]
        put(a_s, ds, pm * sigmoid(p[:c]) * p[c : 2 * c])
        put(b_s, ds, pm * sigmoid(p[2 * c : 3 * c]) * p[3 * c :])

    @pl.loop(0, chunks)
    def _(k):
        project(k)

    @pl.loop(0, chunks)
    def _(k):
        ds = lanes_of(k)
        gate[:, ds] = sigmoid(tn(out_gate[...], normed[:, ds]))
        cot_t[:, ds] = cot[ds, :].astype(F32).T

    pl.semaphore_wait(barrier, n - 1)
    for h in range(parts):
        @pl.loop(0, chunks)
        def _(k):
            near(A_OUT, a_s, a_r, h, k)
            far(B_OUT, b_s, b_r, h, k)

    for h in range(parts):
        @pl.loop(0, chunks)
        def _(k):
            collect(A_OUT, a_r, h, k)
            to_slab(a_r, slab_a, h, k)
            collect(B_OUT, b_r, h, k)
            to_slab(b_r, slab_b, h, k)

        for ch in range(h * hs, (h + 1) * hs):
            keep(slab_o, ch, nt(matrix(slab_a, ch, half), matrix(slab_b, ch, res)))

        @pl.loop(0, chunks)
        def _(k):
            from_slab(slab_o, x_s, h, k)
            near(X_OUT, x_s, x_r, h, k)

    @pl.loop(0, chunks)
    def _(k):
        ds = lanes_of(k)
        for h in range(parts):
            collect(X_OUT, x_r, h, k)
        hat, _ = norm_stats(take(x_r, ds))
        y = (hat * g_om).astype(BF16)
        v = (start[:, ds] + gate[:, ds] * tn(out_final[...], y)).astype(BF16)
        mid[:, ds] = v
        hat, _ = norm_stats(v.astype(F32))
        nb = (hat * g_in).astype(BF16)
        normed[:, ds] = nb
        p = tn(in_proj[...], nb)
        in_p[:, ds] = p
        pm = masks[0:1, ds]
        put(a2_s, ds, pm * sigmoid(p[:c]) * p[c : 2 * c])
        put(b2_s, ds, pm * sigmoid(p[2 * c : 3 * c]) * p[3 * c :])
        near(A_IN, a2_s, a2_r, 0, k)
        near(B_IN, b2_s, b2_r, 0, k)

    for h in range(1, parts):
        @pl.loop(0, chunks)
        def _(k):
            near(A_IN, a2_s, a2_r, h, k)
            near(B_IN, b2_s, b2_r, h, k)

    @pl.loop(0, chunks)
    def _(k):
        ds = lanes_of(k)
        s = sigmoid(tn(in_gate[...], normed[:, ds]))
        logit_s[:, ds] = s
        v = (cot_t[:, ds] * s).astype(BF16)
        gv[:, ds] = v
        gy[:, ds] = nn(in_final[...], v)

    acc_p[...] = jnp.zeros_like(acc_p)
    acc_g[...] = jnp.zeros_like(acc_g)
    acc_f[...] = jnp.zeros_like(acc_f)
    acc_n[...] = jnp.zeros_like(acc_n)
    acc_m[...] = jnp.zeros_like(acc_m)

    for h in range(parts):
        @pl.loop(0, chunks)
        def _(k):
            collect(A_IN, a2_r, h, k)
            to_slab(a2_r, slab_a, h, k)
            collect(B_IN, b2_r, h, k)
            to_slab(b2_r, slab_b, h, k)

        for ch in range(h * hs, (h + 1) * hs):
            a = matrix(slab_a, ch, half)
            b = matrix(slab_b, ch, half)
            mat_a[ch] = a
            mat_b[ch] = b
            keep(slab_o, ch, tn(a, b))

        @pl.loop(0, chunks)
        def _(k):
            from_slab(slab_o, x2_s, h, k)
            far(X_IN, x2_s, x2_r, h, k, True)

    @pl.loop(0, chunks)
    def _(k):
        ds = lanes_of(k)
        for h in range(parts):
            collect(X_IN, x2_r, h, k)
        hat, inv = norm_stats(take_sum(x2_r, ds))
        y = (hat * g_im).astype(BF16)
        value = tn(in_final[...], y)
        s = logit_s[:, ds]
        grad_l = (cot_t[:, ds] * value * s * (1.0 - s)).astype(BF16)
        gl[:, ds] = grad_l
        g = gy[:, ds]
        acc_m[...] += lane_sum(g * hat)
        put(gx_s, ds, norm_back(g, hat, inv, g_im))
        far(G_X, gx_s, gx_r, 0, k)
        acc_f[...] += nt(y, gv[:, ds])

    for h in range(1, parts):
        @pl.loop(0, chunks)
        def _(k):
            far(G_X, gx_s, gx_r, h, k)

    @pl.loop(0, chunks)
    def _(k):
        ds = lanes_of(k)
        grad_l = gl[:, ds]
        acc_g[...] += nt(normed[:, ds], grad_l)
        gy[:, ds] = nn(in_gate[...], grad_l)

    h_s[...] = early().reshape(n, per, 2 * c).astype(BF16)
    spread(H_SUM, h_s, h_r)

    for h in range(parts):
        @pl.loop(0, chunks)
        def _(k):
            collect(G_X, gx_r, h, k)
            to_slab(gx_r, slab_a, h, k)

        for ch in range(h * hs, (h + 1) * hs):
            gx = matrix(slab_a, ch, res)
            keep(slab_o, ch, nt(mat_b[ch], gx))
            keep(slab_b, ch, nn(mat_a[ch], gx))

        @pl.loop(0, chunks)
        def _(k):
            from_slab(slab_o, ga_s, h, k)
            near(G_A, ga_s, ga_r, h, k)
            from_slab(slab_b, gb_s, h, k)
            near(G_B, gb_s, gb_r, h, k)

    gather(H_SUM, h_r)
    hand_round(H_ALL, h_r, u_s, u_r)

    @pl.loop(0, chunks)
    def _(k):
        ds = lanes_of(k)
        for h in range(parts):
            collect(G_A, ga_r, h, k)
            collect(G_B, gb_r, h, k)
        pm = masks[0:1, ds]
        s0 = sigmoid(in_p[:c, ds])
        s2 = sigmoid(in_p[2 * c : 3 * c, ds])
        ga = take(ga_r, ds) * pm * s0
        gb = take(gb_r, ds) * pm * s2
        q0 = (ga * in_p[c : 2 * c, ds] * (1.0 - s0)).astype(BF16)
        q2 = (gb * in_p[3 * c :, ds] * (1.0 - s2)).astype(BF16)
        q = jnp.concatenate([q0, ga.astype(BF16), q2, gb.astype(BF16)], axis=0)
        in_q[:, ds] = q
        acc_p[...] += nt(normed[:, ds], q)

    g_s[...] = (acc_p[...] * inv_count).reshape(n, per, 4 * c).astype(BF16)
    spread(P_SUM, g_s, g_r)

    @pl.loop(0, chunks)
    def _(k):
        ds = lanes_of(k)
        g = nn(in_proj[...], in_q[:, ds]) + gy[:, ds]
        hat, inv = norm_stats(mid[:, ds].astype(F32))
        acc_n[...] += lane_sum(g * hat)
        z = cot_t[:, ds] + norm_back(g, hat, inv, g_in)
        grad_out[ds, :] = z.T.astype(BF16)

    lane = lax.broadcasted_iota(jnp.int32, (c, LANES), 1)
    gains = jnp.where(lane == 0, acc_n[...], jnp.where(lane == 1, acc_m[...], 0.0))
    w_s[...] = (gains * inv_count).T[:8]
    for p in range(1, n):
        copy_to(flag(GAINS), w_s, w_r.at[me], lax.rem(me + p, n)).start()
    w_r[me] = w_s[...]
    gather(P_SUM, g_r)
    hand_round(P_ALL, g_r, t_s, t_r)
    both = gathered(H_ALL, u_r)
    gg_out[...] = both[:, :c]
    gf_out[...] = both[:, c:]
    gather(GAINS, w_r)
    gain_sums = jnp.sum(w_r[...], axis=0)
    gn_out[...] = gain_sums[0:1]
    gm_out[...] = gain_sums[1:2]
    gp_out[...] = gathered(P_ALL, t_r)


def write_out(*refs):
    sems = refs[-1]
    copies = [pltpu.make_async_copy(refs[q], refs[q + 6], sems.at[q]) for q in range(6)]
    for copy in copies:
        copy.start()
    for copy in copies:
        copy.wait()


def shards(n, pair, cotangent, residue_mask, chain_ids, chain_embed, out_norm_gain, out_proj,
           out_gate, out_mid_gain, out_final, in_norm_gain, in_proj, in_gate, in_mid_gain, in_final):
    rows, res, c = pair.shape
    total = rows * res
    per = c // n
    lc = res * min(
        q for q in range(1, rows + 1)
        if rows % q == 0 and q * res % LANES == 0 and (rows // q <= 3)
    )
    tiles = -(-res // LANES)
    def full(dtype):
        return pltpu.VMEM((c, total), dtype)

    m = n // 2
    hc = c // m
    parts = 2 if hc % 32 == 0 else 1
    pitch = hc + PAD
    swap = pltpu.VMEM((m, parts, hc // parts, total), BF16)
    whole = pltpu.VMEM((n, parts, hc // parts, total), BF16)
    slab = pltpu.VMEM((tiles, res * pitch, LANES), F32)
    mats = pltpu.VMEM((hc, m * rows, res), BF16)
    wide = 4 * c
    scratch = [
        pltpu.VMEM((c, 8), F32), pltpu.VMEM((2, total), F32), pltpu.VMEM((4 * c, total), BF16), full(F32), full(BF16), full(F32),
        pltpu.VMEM((4 * c, total), F32), full(F32), full(BF16), full(F32), full(BF16), full(F32),
        full(BF16),
    ] + [
        swap, swap, swap, swap, whole, swap,
        swap, swap, whole, swap, swap, whole,
        swap, whole, swap, swap, swap, swap,
    ] + [slab] * 3 + [mats] * 2 + [
        pltpu.VMEM((c, 4 * c), F32), pltpu.VMEM((c, c), F32), pltpu.VMEM((c, c), F32),
        pltpu.VMEM((c, 1), F32), pltpu.VMEM((c, 1), F32),
        pltpu.VMEM((n, per, wide), BF16), pltpu.VMEM((n, per, wide), BF16),
        pltpu.VMEM((per, wide), BF16), pltpu.VMEM((n, per, wide), BF16),
        pltpu.VMEM((n, per, 2 * c), BF16), pltpu.VMEM((n, per, 2 * c), BF16),
        pltpu.VMEM((per, 2 * c), BF16), pltpu.VMEM((n, per, 2 * c), BF16),
        pltpu.VMEM((8, c), F32), pltpu.VMEM((n, 8, c), F32),
        pltpu.SemaphoreType.DMA((14 * parts * (total // lc),)), pltpu.SemaphoreType.DMA((14 * parts * (total // lc),)),
    ]
    vmem = pl.BlockSpec(memory_space=pltpu.VMEM)
    results = pl.pallas_call(
        functools.partial(kernel, n, rows, res, lc, pitch),
        out_shape=(
            pltpu.VMEM((total, c), BF16),
            pltpu.VMEM((c, 4 * c), F32),
            pltpu.VMEM((c, c), F32),
            pltpu.VMEM((c, c), F32),
            pltpu.VMEM((1, c), F32),
            pltpu.VMEM((1, c), F32),
        ),
        in_specs=[vmem] * 15,
        out_specs=(vmem,) * 6,
        scratch_shapes=scratch,
        compiler_params=pltpu.CompilerParams(
            collective_id=0, has_side_effects=True, vmem_limit_bytes=56 * 1024 * 1024
        ),
    )(
        pair.reshape(total, c), cotangent.reshape(total, c),
        residue_mask.reshape(1, res), chain_ids.reshape(1, res), chain_embed,
        out_norm_gain.reshape(1, c), out_mid_gain.reshape(1, c),
        in_norm_gain.reshape(1, c), in_mid_gain.reshape(1, c),
        out_proj, out_gate, out_final, in_proj, in_gate, in_final,
    )
    shapes = [((total, c), BF16), ((c, 4 * c), F32), ((c, c), F32), ((c, c), F32), ((1, c), F32), ((1, c), F32)]
    grad, gp, gg, gf, gn, gm = pl.pallas_call(
        write_out,
        out_shape=[jax.ShapeDtypeStruct(*shape) for shape in shapes],
        in_specs=[pl.BlockSpec(memory_space=pltpu.VMEM)] * 6,
        out_specs=[pl.BlockSpec(memory_space=pl.ANY)] * 6,
        scratch_shapes=[pltpu.SemaphoreType.DMA((6,))],
    )(*[pltpu.with_memory_space_constraint(r, pltpu.VMEM) for r in results])
    return grad.reshape(rows, res, c), gp, gg, gf, gn.reshape(c), gm.reshape(c)


def solution(mesh):
    split = P("dap", "cplx", None)
    return jax.shard_map(
        functools.partial(shards, mesh.shape["dap"]),
        mesh=mesh,
        in_specs=(split, split, P("cplx"), P("cplx")) + (P(),) * 11,
        out_specs=(split, P("cplx", None), P("cplx", None), P("cplx", None), P("cplx"), P("cplx")),
        check_vma=False,
    )
```

```python
import functools

import jax
import jax.numpy as jnp
from jax import lax
from jax.experimental import pallas as pl
from jax.experimental.pallas import tpu as pltpu
from jax.sharding import PartitionSpec as P

F32 = jnp.float32
BF16 = jnp.bfloat16
LANES = 128
PAD = 8
ALL = (slice(None),)
A_OUT, B_OUT, X_OUT, AB_H, X_H, G_H, D_H, AB_E, X_E, G_E, D_E, GAINS, P_SUM, P_ALL, T_NEAR, T_OVER, T_BACK = range(17)


def tn(w, x):
    return lax.dot_general(w, x, (((0,), (0,)), ((), ())), preferred_element_type=F32)


def nn(w, x):
    return jnp.dot(w, x, preferred_element_type=F32)


def nt(w, x):
    return lax.dot_general(w, x, (((1,), (1,)), ((), ())), preferred_element_type=F32)


def sigmoid(v):
    return 1.0 / (1.0 + jnp.exp(-v))


def norm_stats(v):
    centred = v - jnp.mean(v, axis=0, keepdims=True)
    inv = lax.rsqrt(jnp.mean(centred * centred, axis=0, keepdims=True) + 1e-05)
    return centred * inv, inv


def norm_back(grad, hat, inv, gain):
    scaled = grad * gain
    m1 = jnp.mean(scaled, axis=0, keepdims=True)
    m2 = jnp.mean(scaled * hat, axis=0, keepdims=True)
    return inv * (scaled - m1 - hat * m2)


def lane_sum(v):
    return jnp.sum(v, axis=1, keepdims=True)


def receive_slots(parts, chunks):
    counts = [parts, parts, parts - 1 + chunks] + [chunks] * 8 + [1, 1, 1, 2, 2, 2]
    return [sum(counts[:q]) for q in range(len(counts) + 1)]


def kernel(
    n, rows, res, lc, pitch, every,
    pair_h, cot_h, residues_h, chains_h, embed_h, gain_on_h, gain_om_h, gain_in_h, gain_im_h,
    out_proj_h, out_gate_h, out_final_h, in_proj_h, in_gate_h, in_final_h,
    grad_out, gp_out, gg_out, gf_out, gn_out, gm_out,
    pair, cot, residues, chains, embed, gain_on, gain_om, gain_in, gain_im,
    out_proj, out_gate, out_final, in_proj, in_gate, in_final,
    cols, masks, in_q, start, normed, gate, in_p, cot_t, mid, logit_s, gv, gy, gl,
    a_s, b_s, x_s, a_r, b_r, x_r,
    abh_s, abh_r, xh_s, xh_r, gh_s, gh_r, dh_s, dh_r,
    abe_s, abe_r, xe_s, xe_r, ge_s, ge_r, de_s, de_r,
    slab_a, slab_b, slab_o, mat_a, mat_b, mate_a, mate_b,
    acc_p, acc_g, acc_f, acc_n, acc_m, g_s, g_r, t_s, t_r,
    h_s, h_r, h_own, h_other, h_mean, h_back, f_s, f_r, f_own, f_other, f_mean, f_back, w_s, w_r,
    in_sem, send_sem, recv_sem,
):
    me = lax.axis_index("dap")
    c = start.shape[0]
    per = c // n
    m = n // 2
    parts, hs = a_s.shape[0], a_s.shape[2]
    mine = lax.rem(me, m)
    base = me - mine
    away = m - base
    half = m * rows
    total = rows * res
    chunks = total // lc
    crows = lc // res
    tiles = -(-res // LANES)
    inv_count = 1.0 / res
    we, wh = every // n, (c - every) // m
    groups = ([(0, every)] if every else []) + [(every, c - every)]

    barrier = pltpu.get_barrier_semaphore()
    for p in range(1, n):
        pl.semaphore_signal(
            barrier, inc=1, device_id={"dap": lax.rem(me + p, n)},
            device_id_type=pl.DeviceIdType.MESH,
        )
    sources = [
        pair_h, embed_h, gain_on_h, gain_om_h, gain_in_h, gain_im_h, residues_h, chains_h, out_proj_h,
        out_gate_h, cot_h, out_final_h, in_proj_h, in_gate_h, in_final_h,
    ]
    targets = [
        pair, embed, gain_on, gain_om, gain_in, gain_im, residues, chains, out_proj,
        out_gate, cot, out_final, in_proj, in_gate, in_final,
    ]
    loads = [pltpu.make_async_copy(a, b, in_sem.at[q]) for q, (a, b) in enumerate(zip(sources, targets))]
    for load in loads:
        load.start()

    first_of = receive_slots(parts, chunks)

    def copy_to(which, k, src, dst, peer):
        return pltpu.make_async_remote_copy(
            src_ref=src, dst_ref=dst, send_sem=send_sem.at[which], recv_sem=recv_sem.at[first_of[which] + k],
            device_id={"dap": peer}, device_id_type=pl.DeviceIdType.MESH,
        )

    def lanes_of(k):
        return pl.ds(pl.multiple_of(k * lc, lc), lc)

    def near(which, key, src, dst, lead, ds):
        for p in range(1, m):
            slot = lax.rem(mine + p, m)
            copy_to(which, key, src.at[(*lead, slot, slice(None), ds)], dst.at[(*lead, mine, slice(None), ds)], base + slot).start()
        dst[(*lead, mine, slice(None), ds)] = src[(*lead, mine, slice(None), ds)]

    def far(which, key, src, dst, lead, ds, by_peer=False):
        for first, other in ((0, True), (1, False)):
            for p in range(first, m):
                slot = lax.rem(mine + p, m)
                peer = (away if other else base) + slot
                at = peer if by_peer else slot
                copy_to(which, key, src.at[(*lead, at, slice(None), ds)], dst.at[(*lead, me, slice(None), ds)], peer).start()
        dst[(*lead, me, slice(None), ds)] = src[(*lead, me if by_peer else mine, slice(None), ds)]

    def across(which, key, src, dst, lead, ds, other):
        for p in range(0 if other else 1, m):
            peer = (away if other else base) + lax.rem(mine + p, m)
            copy_to(which, key, src.at[(*lead, peer, slice(None), ds)], dst.at[(*lead, me, slice(None), ds)], peer).start()
        if not other:
            dst[(*lead, me, slice(None), ds)] = src[(*lead, me, slice(None), ds)]

    def arrived(which, key, block):
        copy_to(which, key, block, block, lax.rem(me + 1, n)).wait_recv()

    def sent(which, block):
        copy_to(which, 0, block, block, lax.rem(me + 1, n)).wait_send()

    def spread(which, key, src, dst):
        for p in range(1, n):
            peer = lax.rem(me + p, n)
            copy_to(which, key, src.at[peer], dst.at[me], peer).start()
        dst[me] = src[me]

    def put(ref, lead, ds, value, count, width):
        ref[(*lead, slice(None), slice(None), ds)] = value.reshape(count, width, lc).astype(BF16)

    def take(ref, lead, ds):
        block = ref[(*lead, slice(None), slice(None), ds)].astype(F32)
        return block.reshape(block.shape[0] * block.shape[1], lc)

    def to_slab(ref, lead, slab, slot, k):
        ds = lanes_of(k)
        width_c = ref.shape[-2]
        for s in range(ref.shape[-3]):
            block = ref[(*lead, s, slice(None), ds)].astype(F32)
            row = s * rows + k * crows
            for i in range(crows):
                part = block[:, i * res : (i + 1) * res]
                at = pl.ds(pl.multiple_of((row + i) * pitch + slot, 8), width_c)
                for t in range(tiles):
                    width = min(LANES, res - t * LANES)
                    slab[t, at, :width] = part[:, t * LANES : t * LANES + width]

    def matrix(slab, ch, count):
        at = pl.ds(ch, count, stride=pitch)
        pieces = [slab[t, at, :] for t in range(tiles)]
        whole = pieces[0] if tiles == 1 else jnp.concatenate(pieces, axis=1)
        return whole[:, :res].astype(BF16)

    def keep(slab, ch, value):
        count = value.shape[0]
        pad = tiles * LANES - res
        if pad:
            value = jnp.concatenate([value, jnp.zeros((count, pad), F32)], axis=1)
        for t in range(tiles):
            slab[t, pl.ds(ch, count, stride=pitch), :] = value[:, t * LANES : (t + 1) * LANES]

    def from_slab(slab, slot, ref, lead, k):
        width_c = ref.shape[-2]
        for s in range(ref.shape[-3]):
            row = s * rows + k * crows
            pieces = []
            for i in range(crows):
                at = pl.ds(pl.multiple_of((row + i) * pitch + slot, 8), width_c)
                for t in range(tiles):
                    width = min(LANES, res - t * LANES)
                    pieces.append(slab[t, at, :width])
            ref[(*lead, s, slice(None), lanes_of(k))] = jnp.concatenate(pieces, axis=1).astype(BF16)

    def early():
        return jnp.concatenate([acc_g[...], acc_f[...]], axis=1) * inv_count

    def hand_round(which, key, src, own, dst):
        summed = jnp.sum(src.astype(F32), axis=0).astype(BF16)
        own[...] = summed
        for p in range(1, n):
            copy_to(which, key, own, dst.at[me], lax.rem(me + p, n)).start()
        dst[me] = summed

    def level_near(key, rows_of, got):
        for p in range(1, m):
            slot = lax.rem(mine + p, m)
            copy_to(T_NEAR, key, rows_of.at[slot], got.at[mine], base + slot).start()
        got[mine] = rows_of[mine]

    def level_over(key, got, own, other):
        arrived(T_NEAR, key, got.at[pl.ds(0, m - 1)])
        own[...] = jnp.sum(got[...].astype(F32), axis=0).astype(BF16)
        copy_to(T_OVER, key, own, other, away + mine).start()

    def level_back(key, own, other, mean, back):
        arrived(T_OVER, key, other)
        mean[...] = (own[...].astype(F32) + other[...].astype(F32)).astype(BF16)
        for p in range(1, m):
            copy_to(T_BACK, key, mean, back.at[mine], base + lax.rem(mine + p, m)).start()
        back[mine] = mean[...]

    def level_sent(key_refs):
        for got, other, back in key_refs:
            sent(T_NEAR, got.at[pl.ds(0, m - 1)])
            sent(T_OVER, other)
            sent(T_BACK, back.at[pl.ds(0, m - 1)])

    for load in loads[:8]:
        load.wait()
    params = [embed[...], gain_on[...], gain_om[...], gain_in[...], gain_im[...]]
    cols[...] = jnp.concatenate(params + [jnp.zeros((2, c), F32)], axis=0).T
    here = lax.broadcasted_iota(jnp.int32, (rows, res), 1) == (
        lax.broadcasted_iota(jnp.int32, (rows, res), 0) + me * rows
    )
    row_mask = jnp.sum(jnp.where(here, residues[...], 0).astype(F32), axis=1, keepdims=True)
    row_chain = jnp.sum(jnp.where(here, chains[...], 0).astype(F32), axis=1, keepdims=True)
    both = row_mask * residues[...].astype(F32)
    same_chain = jnp.where(row_chain == chains[...].astype(F32), 1.0, 0.0)
    masks[0:1, :] = jnp.concatenate([both[i : i + 1] for i in range(rows)], axis=1)
    masks[1:2, :] = jnp.concatenate([same_chain[i : i + 1] for i in range(rows)], axis=1)
    emb0, emb1 = cols[:, 0:1], cols[:, 1:2]
    g_on, g_om, g_in, g_im = (cols[:, q : q + 1] for q in range(2, 6))
    loads[8].wait()

    def project(k):
        ds = lanes_of(k)
        same = masks[1:2, ds] > 0.5
        x = pair[ds, :].astype(F32).T + jnp.where(same, emb1, emb0)
        start[:, ds] = x
        hat, _ = norm_stats(x)
        nb = (hat * g_on).astype(BF16)
        normed[:, ds] = nb
        p = tn(out_proj[...], nb)
        pm = masks[0:1, ds]
        left = pm * sigmoid(p[:c]) * p[c : 2 * c]
        right = pm * sigmoid(p[2 * c : 3 * c]) * p[3 * c :]
        a_s[:, :, :, ds] = left.reshape(parts, m, hs, lc).astype(BF16)
        b_s[:, :, :, ds] = right.reshape(parts, m, hs, lc).astype(BF16)

    @pl.loop(0, chunks)
    def _(k):
        project(k)

    pl.semaphore_wait(barrier, n - 1)

    @pl.loop(0, parts)
    def _(h):
        near(A_OUT, h, a_s, a_r, (h,), pl.ds(0, total))
        far(B_OUT, h, b_s, b_r, (h,), pl.ds(0, total))

    for load in loads[9:]:
        load.wait()

    @pl.loop(0, chunks)
    def _(k):
        ds = lanes_of(k)
        gate[:, ds] = sigmoid(tn(out_gate[...], normed[:, ds]))
        cot_t[:, ds] = cot[ds, :].astype(F32).T

    def outgoing(h):
        arrived(A_OUT, h, a_r.at[h, pl.ds(0, m - 1)])

        @pl.loop(0, chunks)
        def _(k):
            to_slab(a_r, (h,), slab_a, h * hs, k)

        arrived(B_OUT, h, b_r.at[h, pl.ds(0, n - 1)])

        @pl.loop(0, chunks)
        def _(k):
            to_slab(b_r, (h,), slab_b, h * hs, k)

        for ch in range(hs):
            at = h * hs + ch
            keep(slab_o, at, nt(matrix(slab_a, at, half), matrix(slab_b, at, res)))

    @pl.loop(0, parts - 1)
    def _(h):
        outgoing(h)

        @pl.loop(0, chunks)
        def _(k):
            from_slab(slab_o, h * hs, x_s, (h,), k)

        near(X_OUT, h, x_s, x_r, (h,), pl.ds(0, total))

    outgoing(parts - 1)

    @pl.loop(0, chunks)
    def _(k):
        from_slab(slab_o, (parts - 1) * hs, x_s, (parts - 1,), k)
        near(X_OUT, parts - 1 + k, x_s, x_r, (parts - 1,), lanes_of(k))

    @pl.loop(0, parts - 1)
    def _(h):
        arrived(X_OUT, h, x_r.at[h, pl.ds(0, m - 1)])

    @pl.loop(0, chunks)
    def _(k):
        ds = lanes_of(k)
        arrived(X_OUT, parts - 1 + k, x_r.at[parts - 1, pl.ds(0, m - 1), :, ds])
        hat, _ = norm_stats(x_r[:, :, :, ds].astype(F32).reshape(c, lc))
        y = (hat * g_om).astype(BF16)
        v = (start[:, ds] + gate[:, ds] * tn(out_final[...], y)).astype(BF16)
        mid[:, ds] = v
        hat, _ = norm_stats(v.astype(F32))
        nb = (hat * g_in).astype(BF16)
        normed[:, ds] = nb
        p = tn(in_proj[...], nb)
        in_p[:, ds] = p
        pm = masks[0:1, ds]
        for q in range(2):
            value = pm * sigmoid(p[2 * q * c : (2 * q + 1) * c]) * p[(2 * q + 1) * c : (2 * q + 2) * c]
            put(abh_s, (q,), ds, value[every:], m, wh)
            if every:
                put(abe_s, (q,), ds, value[:every], n, we)
        near(AB_H, k, abh_s, abh_r, ALL, ds)
        if every:
            @pl.when(k > 0)
            def _():
                across(AB_E, k - 1, abe_s, abe_r, ALL, lanes_of(k - 1), True)

    if every:
        across(AB_E, chunks - 1, abe_s, abe_r, ALL, lanes_of(chunks - 1), True)

        @pl.loop(0, chunks)
        def _(k):
            across(AB_E, k, abe_s, abe_r, ALL, lanes_of(k), False)

    @pl.loop(0, chunks)
    def _(k):
        ds = lanes_of(k)
        s = sigmoid(tn(in_gate[...], normed[:, ds]))
        logit_s[:, ds] = s
        v = (cot_t[:, ds] * s).astype(BF16)
        gv[:, ds] = v
        gy[:, ds] = nn(in_final[...], v)

    acc_p[...] = jnp.zeros_like(acc_p)
    acc_g[...] = jnp.zeros_like(acc_g)
    acc_f[...] = jnp.zeros_like(acc_f)
    acc_n[...] = jnp.zeros_like(acc_n)
    acc_m[...] = jnp.zeros_like(acc_m)

    @pl.loop(0, chunks)
    def _(k):
        ds = lanes_of(k)
        arrived(AB_H, k, abh_r.at[:, pl.ds(0, m - 1), :, ds])
        to_slab(abh_r, (0,), slab_a, we, k)
        to_slab(abh_r, (1,), slab_b, we, k)

    for ch in range(wh):
        a = matrix(slab_a, we + ch, half)
        b = matrix(slab_b, we + ch, half)
        mat_a[ch] = a
        mat_b[ch] = b
        keep(slab_o, we + ch, tn(a, b))

    early_chunks = chunks - 1 if every else chunks

    @pl.loop(0, early_chunks)
    def _(k):
        from_slab(slab_o, we, xh_s, (), k)
        far(X_H, k, xh_s, xh_r, (), lanes_of(k), True)

    if every:
        from_slab(slab_o, we, xh_s, (), early_chunks)

        @pl.loop(0, chunks)
        def _(k):
            ds = lanes_of(k)
            arrived(AB_E, k, abe_r.at[:, pl.ds(0, n - 1), :, ds])
            to_slab(abe_r, (0,), slab_a, 0, k)
            to_slab(abe_r, (1,), slab_b, 0, k)

        for ch in range(we):
            a = matrix(slab_a, ch, res)
            b = matrix(slab_b, ch, res)
            mate_a[ch] = a
            mate_b[ch] = b
            keep(slab_o, ch, tn(a, b))

        def send_x(k):
            from_slab(slab_o, 0, xe_s, (), k)
            across(X_E, k, xe_s, xe_r, (), lanes_of(k), True)
            across(X_E, k, xe_s, xe_r, (), lanes_of(k), False)

        send_x(0)
        far(X_H, early_chunks, xh_s, xh_r, (), lanes_of(early_chunks), True)

        @pl.loop(1, chunks)
        def _(k):
            send_x(k)

    @pl.loop(0, chunks)
    def _(k):
        ds = lanes_of(k)
        arrived(X_H, k, xh_r.at[pl.ds(0, n - 1), :, ds])
        both = xh_r[pl.ds(0, m), :, ds].astype(F32) + xh_r[pl.ds(m, m), :, ds].astype(F32)
        x = both.reshape(c - every, lc)
        if every:
            arrived(X_E, k, xe_r.at[pl.ds(0, n - 1), :, ds])
            x = jnp.concatenate([take(xe_r, (), ds), x], axis=0)
        hat, inv = norm_stats(x)
        y = (hat * g_im).astype(BF16)
        value = tn(in_final[...], y)
        s = logit_s[:, ds]
        grad_l = (cot_t[:, ds] * value * s * (1.0 - s)).astype(BF16)
        gl[:, ds] = grad_l
        g = gy[:, ds]
        acc_m[...] += lane_sum(g * hat)
        grad_x = norm_back(g, hat, inv, g_im)
        put(gh_s, (), ds, grad_x[every:], m, wh)
        if every:
            put(ge_s, (), ds, grad_x[:every], n, we)
            across(G_E, k, ge_s, ge_r, (), ds, True)
            across(G_E, k, ge_s, ge_r, (), ds, False)
        else:
            far(G_H, k, gh_s, gh_r, (), ds)
        acc_f[...] += nt(y, gv[:, ds])

    if every:
        @pl.loop(0, chunks)
        def _(k):
            far(G_H, k, gh_s, gh_r, (), lanes_of(k))

    @pl.loop(0, chunks)
    def _(k):
        ds = lanes_of(k)
        grad_l = gl[:, ds]
        acc_g[...] += nt(normed[:, ds], grad_l)
        gy[:, ds] = nn(in_gate[...], grad_l)

    h_s[...] = early().reshape(m, c // m, 2 * c).astype(BF16)
    level_near(0, h_s, h_r)

    if every:
        @pl.loop(0, chunks)
        def _(k):
            arrived(G_E, k, ge_r.at[pl.ds(0, n - 1), :, lanes_of(k)])
            to_slab(ge_r, (), slab_a, 0, k)

        for ch in range(we):
            gx = matrix(slab_a, ch, res)
            keep(slab_o, ch, nt(mate_b[ch], gx))
            keep(slab_b, ch, nn(mate_a[ch], gx))

        @pl.loop(0, chunks)
        def _(k):
            ds = lanes_of(k)
            for q, slab in enumerate((slab_o, slab_b)):
                from_slab(slab, 0, de_s, (q,), k)
            across(D_E, k, de_s, de_r, ALL, ds, True)
            across(D_E, k, de_s, de_r, ALL, ds, False)

    @pl.loop(0, chunks)
    def _(k):
        arrived(G_H, k, gh_r.at[pl.ds(0, n - 1), :, lanes_of(k)])
        to_slab(gh_r, (), slab_a, we, k)

    for ch in range(wh):
        gx = matrix(slab_a, we + ch, res)
        keep(slab_o, we + ch, nt(mat_b[ch], gx))
        keep(slab_b, we + ch, nn(mat_a[ch], gx))

    @pl.loop(0, chunks)
    def _(k):
        for q, slab in enumerate((slab_o, slab_b)):
            from_slab(slab, we, dh_s, (q,), k)
        near(D_H, k, dh_s, dh_r, ALL, lanes_of(k))

    level_over(0, h_r, h_own, h_other)
    for g, (first, count) in enumerate(groups):
        @pl.loop(0, chunks)
        def _(k):
            ds = lanes_of(k)
            if first:
                arrived(D_H, k, dh_r.at[:, pl.ds(0, m - 1), :, ds])
                grads = [take(dh_r, (q,), ds) for q in range(2)]
            elif every:
                arrived(D_E, k, de_r.at[:, pl.ds(0, n - 1), :, ds])
                grads = [take(de_r, (q,), ds) for q in range(2)]
            else:
                arrived(D_H, k, dh_r.at[:, pl.ds(0, m - 1), :, ds])
                grads = [take(dh_r, (q,), ds) for q in range(2)]
            pm = masks[0:1, ds]
            blocks = []
            for q in range(2):
                s = sigmoid(in_p[pl.ds(2 * q * c + first, count), ds])
                scaled = grads[q] * pm * s
                blocks.append((scaled * in_p[pl.ds((2 * q + 1) * c + first, count), ds] * (1.0 - s)).astype(BF16))
                blocks.append(scaled.astype(BF16))
            for b in range(4):
                in_q[pl.ds(b * c + first, count), ds] = blocks[b]
            acc_p[g] += nt(normed[:, ds], jnp.concatenate(blocks, axis=0))

        if g == 0 and every:
            f_s[...] = (acc_p[g] * inv_count).reshape(m, c // m, 4 * count).astype(BF16)
            level_near(1, f_s, f_r)
            level_back(0, h_own, h_other, h_mean, h_back)
        else:
            g_s[...] = (acc_p[g] * inv_count).reshape(n, per, 4 * count).astype(BF16)
            spread(P_SUM, 0, g_s, g_r)
    if every:
        level_over(1, f_r, f_own, f_other)
    else:
        level_back(0, h_own, h_other, h_mean, h_back)

    @pl.loop(0, chunks)
    def _(k):
        ds = lanes_of(k)
        g = nn(in_proj[...], in_q[:, ds]) + gy[:, ds]
        hat, inv = norm_stats(mid[:, ds].astype(F32))
        acc_n[...] += lane_sum(g * hat)
        z = cot_t[:, ds] + norm_back(g, hat, inv, g_in)
        grad_out[ds, :] = z.T.astype(BF16)

    lane = lax.broadcasted_iota(jnp.int32, (c, LANES), 1)
    gains = jnp.where(lane == 0, acc_n[...], jnp.where(lane == 1, acc_m[...], 0.0))
    w_s[...] = (gains * inv_count).T[:2]
    for p in range(1, n):
        copy_to(GAINS, 0, w_s, w_r.at[me], lax.rem(me + p, n)).start()
    w_r[me] = w_s[...]
    if every:
        level_back(1, f_own, f_other, f_mean, f_back)
    arrived(P_SUM, 0, g_r.at[pl.ds(0, n - 1)])
    hand_round(P_ALL, 0, g_r[...], t_s, t_r)
    arrived(T_BACK, 0, h_back.at[pl.ds(0, m - 1)])
    both = h_back[...].astype(F32).reshape(c, 2 * c)
    gg_out[...] = both[:, :c]
    gf_out[...] = both[:, c:]
    arrived(GAINS, 0, w_r.at[pl.ds(0, n - 1)])
    gain_sums = jnp.sum(w_r[...], axis=0)
    gn_out[...] = gain_sums[0:1]
    gm_out[...] = gain_sums[1:2]

    for h in range(parts):
        sent(A_OUT, a_r.at[h, pl.ds(0, m - 1)])
        sent(B_OUT, b_r.at[h, pl.ds(0, n - 1)])
        sent(X_OUT, x_r.at[h, pl.ds(0, m - 1)])
    for q in range(2):
        sent(AB_H, abh_r.at[q, pl.ds(0, m - 1)])
        sent(D_H, dh_r.at[q, pl.ds(0, m - 1)])
    sent(X_H, xh_r.at[pl.ds(0, n - 1)])
    sent(G_H, gh_r.at[pl.ds(0, n - 1)])
    if every:
        for q in range(2):
            sent(AB_E, abe_r.at[q, pl.ds(0, n - 1)])
            sent(D_E, de_r.at[q, pl.ds(0, n - 1)])
        sent(X_E, xe_r.at[pl.ds(0, n - 1)])
        sent(G_E, ge_r.at[pl.ds(0, n - 1)])
    sent(GAINS, w_r.at[pl.ds(0, n - 1)])
    sent(P_SUM, g_r.at[pl.ds(0, n - 1)])
    level_sent([(h_r, h_other, h_back)] + ([(f_r, f_other, f_back)] if every else []))

    for g, (first, count) in enumerate(groups):
        if g == 0 and every:
            arrived(T_BACK, 1, f_back.at[pl.ds(0, m - 1)])
            whole = f_back[...].astype(F32).reshape(c, 4 * count)
        else:
            arrived(P_ALL, 0, t_r.at[pl.ds(0, n - 1)])
            sent(P_ALL, t_r.at[pl.ds(0, n - 1)])
            whole = t_r[...].astype(F32).reshape(c, 4 * count)
        for b in range(4):
            gp_out[:, b * c + first : b * c + first + count] = whole[:, b * count : (b + 1) * count]


def write_out(*refs):
    sems = refs[-1]
    copies = [pltpu.make_async_copy(refs[q], refs[q + 6], sems.at[q]) for q in range(6)]
    for copy in copies:
        copy.start()
    for copy in copies:
        copy.wait()


def shards(n, pair, cotangent, residue_mask, chain_ids, chain_embed, out_norm_gain, out_proj,
           out_gate, out_mid_gain, out_final, in_norm_gain, in_proj, in_gate, in_mid_gain, in_final):
    rows, res, c = pair.shape
    total = rows * res
    per = c // n
    lc = res * min(
        q for q in range(1, rows + 1)
        if rows % q == 0 and q * res % LANES == 0 and (rows // q <= 3)
    )
    tiles = -(-res // LANES)
    def full(dtype):
        return pltpu.VMEM((c, total), dtype)

    def block(*shape):
        return pltpu.VMEM((*shape, total), BF16)

    m = n // 2
    hc = c // m
    parts = hc // 8 if hc % 8 == 0 else 1
    every = c // 2 if (c // 2) % (8 * n) == 0 else 0
    we, wh = max(every // n, 8), (c - every) // m
    groups = 2 if every else 1
    wide = 4 * c // groups
    pitch = max(hc, every // n + wh) + PAD
    hs = hc // parts
    chunks = total // lc
    slab = pltpu.VMEM((tiles, res * pitch, LANES), F32)
    small = n if every else 1
    scratch = [
        pltpu.VMEM((total, c), BF16), pltpu.VMEM((total, c), BF16), pltpu.VMEM((1, res), jnp.int32), pltpu.VMEM((1, res), jnp.int32),
        pltpu.VMEM((2, c), F32),
    ] + [pltpu.VMEM((1, c), F32)] * 4 + [
        pltpu.VMEM((c, 4 * c), BF16), pltpu.VMEM((c, c), BF16), pltpu.VMEM((c, c), BF16),
        pltpu.VMEM((c, 4 * c), BF16), pltpu.VMEM((c, c), BF16), pltpu.VMEM((c, c), BF16),
        pltpu.VMEM((c, 8), F32), pltpu.VMEM((2, total), F32), pltpu.VMEM((4 * c, total), BF16), full(F32), full(BF16), full(F32),
        pltpu.VMEM((4 * c, total), F32), full(F32), full(BF16), full(F32), full(BF16), full(F32), full(BF16),
        block(parts, m, hs), block(parts, m, hs), block(parts, m, hs),
        block(parts, m, hs), block(parts, n, hs), block(parts, m, hs),
        block(2, m, wh), block(2, m, wh), block(n, wh), block(n, wh),
        block(m, wh), block(n, wh), block(2, m, wh), block(2, m, wh),
        block(2, small, we), block(2, small, we), block(small, we), block(small, we),
        block(small, we), block(small, we), block(2, small, we), block(2, small, we),
        slab, slab, slab,
        pltpu.VMEM((wh, m * rows, res), BF16), pltpu.VMEM((wh, m * rows, res), BF16),
        pltpu.VMEM((we, res, res), BF16), pltpu.VMEM((we, res, res), BF16),
        pltpu.VMEM((groups, c, wide), F32), pltpu.VMEM((c, c), F32), pltpu.VMEM((c, c), F32),
        pltpu.VMEM((c, 1), F32), pltpu.VMEM((c, 1), F32),
        pltpu.VMEM((n, per, wide), BF16), pltpu.VMEM((n, per, wide), BF16),
        pltpu.VMEM((per, wide), BF16), pltpu.VMEM((n, per, wide), BF16),
    ] + [
        pltpu.VMEM(shape, BF16) for w in (2 * c, wide)
        for shape in ((m, hc, w), (m, hc, w), (hc, w), (hc, w), (hc, w), (m, hc, w))
    ] + [
        pltpu.VMEM((2, c), F32), pltpu.VMEM((n, 2, c), F32),
        pltpu.SemaphoreType.DMA((15,)), pltpu.SemaphoreType.DMA((17,)), pltpu.SemaphoreType.DMA((receive_slots(parts, chunks)[-1],)),
    ]
    vmem = pl.BlockSpec(memory_space=pltpu.VMEM)
    results = pl.pallas_call(
        functools.partial(kernel, n, rows, res, lc, pitch, every),
        out_shape=(
            pltpu.VMEM((total, c), BF16),
            pltpu.VMEM((c, 4 * c), F32),
            pltpu.VMEM((c, c), F32),
            pltpu.VMEM((c, c), F32),
            pltpu.VMEM((1, c), F32),
            pltpu.VMEM((1, c), F32),
        ),
        in_specs=[pl.BlockSpec(memory_space=pl.ANY)] * 15,
        out_specs=(vmem,) * 6,
        scratch_shapes=scratch,
        compiler_params=pltpu.CompilerParams(
            collective_id=0, has_side_effects=True, vmem_limit_bytes=56 * 1024 * 1024
        ),
    )(
        pair.reshape(total, c), cotangent.reshape(total, c),
        residue_mask.reshape(1, res), chain_ids.reshape(1, res), chain_embed,
        out_norm_gain.reshape(1, c), out_mid_gain.reshape(1, c),
        in_norm_gain.reshape(1, c), in_mid_gain.reshape(1, c),
        out_proj, out_gate, out_final, in_proj, in_gate, in_final,
    )
    shapes = [((total, c), BF16), ((c, 4 * c), F32), ((c, c), F32), ((c, c), F32), ((1, c), F32), ((1, c), F32)]
    grad, gp, gg, gf, gn, gm = pl.pallas_call(
        write_out,
        out_shape=[jax.ShapeDtypeStruct(*shape) for shape in shapes],
        in_specs=[pl.BlockSpec(memory_space=pltpu.VMEM)] * 6,
        out_specs=[pl.BlockSpec(memory_space=pl.ANY)] * 6,
        scratch_shapes=[pltpu.SemaphoreType.DMA((6,))],
    )(*[pltpu.with_memory_space_constraint(r, pltpu.VMEM) for r in results])
    return grad.reshape(rows, res, c), gp, gg, gf, gn.reshape(c), gm.reshape(c)


def solution(mesh):
    split = P("dap", "cplx", None)
    return jax.shard_map(
        functools.partial(shards, mesh.shape["dap"]),
        mesh=mesh,
        in_specs=(split, split, P("cplx"), P("cplx")) + (P(),) * 11,
        out_specs=(split, P("cplx", None), P("cplx", None), P("cplx", None), P("cplx"), P("cplx")),
        check_vma=False,
    )
```

```python
import functools

import jax
import jax.numpy as jnp
from jax import lax
from jax.experimental import pallas as pl
from jax.experimental.pallas import tpu as pltpu
from jax.sharding import PartitionSpec as P

F32 = jnp.float32
BF16 = jnp.bfloat16
LANES = 128
PAD = 8
ALL = (slice(None),)
A_OUT, B_OUT, X_OUT, AB_H, X_H, G_H, D_H, AB_E, X_E, G_E, D_E, GAINS, P_SUM, P_ALL, T_NEAR, T_OVER, T_BACK = range(17)


def tn(w, x):
    return lax.dot_general(w, x, (((0,), (0,)), ((), ())), preferred_element_type=F32)


def nn(w, x):
    return jnp.dot(w, x, preferred_element_type=F32)


def nt(w, x):
    return lax.dot_general(w, x, (((1,), (1,)), ((), ())), preferred_element_type=F32)


def sigmoid(v):
    return 1.0 / (1.0 + jnp.exp(-v))


def norm_stats(v):
    centred = v - jnp.mean(v, axis=0, keepdims=True)
    inv = lax.rsqrt(jnp.mean(centred * centred, axis=0, keepdims=True) + 1e-05)
    return centred * inv, inv


def norm_back(grad, hat, inv, gain):
    scaled = grad * gain
    m1 = jnp.mean(scaled, axis=0, keepdims=True)
    m2 = jnp.mean(scaled * hat, axis=0, keepdims=True)
    return inv * (scaled - m1 - hat * m2)


def lane_sum(v):
    return jnp.sum(v, axis=1, keepdims=True)


def receive_slots(parts, chunks):
    counts = [parts, parts, parts - 1 + chunks] + [chunks] * 8 + [1, 2, 2, 1, 1, 1]
    return [sum(counts[:q]) for q in range(len(counts) + 1)]


def kernel(
    n, rows, res, lc, pitch, every,
    pair_h, cot_h, residues_h, chains_h, embed_h, gain_on_h, gain_om_h, gain_in_h, gain_im_h,
    out_proj_h, out_gate_h, out_final_h, in_proj_h, in_gate_h, in_final_h,
    grad_out, gp_out, gg_out, gf_out, gn_out, gm_out,
    pair, cot, residues, chains, embed, gain_on, gain_om, gain_in, gain_im,
    out_proj, out_gate, out_final, in_proj, in_gate, in_final,
    cols, masks, in_q, start, normed, gate, in_p, cot_t, mid, logit_s, gv, gy, gl,
    a_s, b_s, x_s, a_r, b_r, x_r,
    abh_s, abh_r, xh_s, xh_r, gh_s, gh_r, dh_s, dh_r,
    abe_s, abe_r, xe_s, xe_r, ge_s, ge_r, de_s, de_r,
    slab_a, slab_b, slab_o, mat_a, mat_b, mate_a, mate_b,
    acc_p, acc_g, acc_f, acc_n, acc_m, g_s, g_r, t_s, t_r,
    h_s, h_r, h_own, h_other, h_mean, h_back, f_s, f_r, f_own, f_back, w_s, w_r,
    in_sem, send_sem, recv_sem,
):
    me = lax.axis_index("dap")
    c = start.shape[0]
    per = c // n
    m = n // 2
    parts, hs = a_s.shape[0], a_s.shape[2]
    mine = lax.rem(me, m)
    base = me - mine
    away = m - base
    half = m * rows
    total = rows * res
    chunks = total // lc
    crows = lc // res
    tiles = -(-res // LANES)
    inv_count = 1.0 / res
    we, wh = every // n, (c - every) // m
    groups = ([(0, every)] if every else []) + [(every, c - every)]

    barrier = pltpu.get_barrier_semaphore()
    for p in range(1, n):
        pl.semaphore_signal(
            barrier, inc=1, device_id={"dap": lax.rem(me + p, n)},
            device_id_type=pl.DeviceIdType.MESH,
        )
    sources = [
        pair_h, embed_h, gain_on_h, gain_om_h, gain_in_h, gain_im_h, residues_h, chains_h, out_proj_h,
        out_gate_h, cot_h, out_final_h, in_proj_h, in_gate_h, in_final_h,
    ]
    targets = [
        pair, embed, gain_on, gain_om, gain_in, gain_im, residues, chains, out_proj,
        out_gate, cot, out_final, in_proj, in_gate, in_final,
    ]
    loads = [pltpu.make_async_copy(a, b, in_sem.at[q]) for q, (a, b) in enumerate(zip(sources, targets))]
    for load in loads:
        load.start()

    first_of = receive_slots(parts, chunks)

    def copy_to(which, k, src, dst, peer):
        return pltpu.make_async_remote_copy(
            src_ref=src, dst_ref=dst, send_sem=send_sem.at[which], recv_sem=recv_sem.at[first_of[which] + k],
            device_id={"dap": peer}, device_id_type=pl.DeviceIdType.MESH,
        )

    def lanes_of(k):
        return pl.ds(pl.multiple_of(k * lc, lc), lc)

    def near(which, key, src, dst, lead, ds):
        for p in range(1, m):
            slot = lax.rem(mine + p, m)
            copy_to(which, key, src.at[(*lead, slot, slice(None), ds)], dst.at[(*lead, mine, slice(None), ds)], base + slot).start()
        dst[(*lead, mine, slice(None), ds)] = src[(*lead, mine, slice(None), ds)]

    def far(which, key, src, dst, lead, ds, by_peer=False):
        for first, other in ((0, True), (1, False)):
            for p in range(first, m):
                slot = lax.rem(mine + p, m)
                peer = (away if other else base) + slot
                at = peer if by_peer else slot
                copy_to(which, key, src.at[(*lead, at, slice(None), ds)], dst.at[(*lead, me, slice(None), ds)], peer).start()
        dst[(*lead, me, slice(None), ds)] = src[(*lead, me if by_peer else mine, slice(None), ds)]

    def across(which, key, src, dst, lead, ds, other):
        for p in range(0 if other else 1, m):
            peer = (away if other else base) + lax.rem(mine + p, m)
            copy_to(which, key, src.at[(*lead, peer, slice(None), ds)], dst.at[(*lead, me, slice(None), ds)], peer).start()
        if not other:
            dst[(*lead, me, slice(None), ds)] = src[(*lead, me, slice(None), ds)]

    def arrived(which, key, block):
        copy_to(which, key, block, block, lax.rem(me + 1, n)).wait_recv()

    def sent(which, block):
        copy_to(which, 0, block, block, lax.rem(me + 1, n)).wait_send()

    def put(ref, lead, ds, value, count, width):
        ref[(*lead, slice(None), slice(None), ds)] = value.reshape(count, width, lc).astype(BF16)

    def take(ref, lead, ds):
        block = ref[(*lead, slice(None), slice(None), ds)].astype(F32)
        return block.reshape(block.shape[0] * block.shape[1], lc)

    def to_slab(ref, lead, slab, slot, k):
        ds = lanes_of(k)
        width_c = ref.shape[-2]
        for s in range(ref.shape[-3]):
            block = ref[(*lead, s, slice(None), ds)].astype(F32)
            row = s * rows + k * crows
            for i in range(crows):
                part = block[:, i * res : (i + 1) * res]
                at = pl.ds(pl.multiple_of((row + i) * pitch + slot, 8), width_c)
                for t in range(tiles):
                    width = min(LANES, res - t * LANES)
                    slab[t, at, :width] = part[:, t * LANES : t * LANES + width]

    def matrix(slab, ch, count):
        at = pl.ds(ch, count, stride=pitch)
        pieces = [slab[t, at, :] for t in range(tiles)]
        whole = pieces[0] if tiles == 1 else jnp.concatenate(pieces, axis=1)
        return whole[:, :res].astype(BF16)

    def keep(slab, ch, value):
        count = value.shape[0]
        pad = tiles * LANES - res
        if pad:
            value = jnp.concatenate([value, jnp.zeros((count, pad), F32)], axis=1)
        for t in range(tiles):
            slab[t, pl.ds(ch, count, stride=pitch), :] = value[:, t * LANES : (t + 1) * LANES]

    def from_slab(slab, slot, ref, lead, k):
        width_c = ref.shape[-2]
        for s in range(ref.shape[-3]):
            row = s * rows + k * crows
            pieces = []
            for i in range(crows):
                at = pl.ds(pl.multiple_of((row + i) * pitch + slot, 8), width_c)
                for t in range(tiles):
                    width = min(LANES, res - t * LANES)
                    pieces.append(slab[t, at, :width])
            ref[(*lead, s, slice(None), lanes_of(k))] = jnp.concatenate(pieces, axis=1).astype(BF16)

    def early():
        return jnp.concatenate([acc_g[...], acc_f[...]], axis=1) * inv_count

    first_mid = n // 4
    in_middle = (me >= first_mid) & (me < first_mid + m)

    def middle_sum(key, src, got):
        for r in range(m):
            @pl.when(me != first_mid + r)
            def _():
                copy_to(P_SUM, key, src.at[r], got.at[me], first_mid + r).start()

        @pl.when(in_middle)
        def _():
            got[me] = src[me - first_mid]

    def middle_round(key, got, own, back):
        @pl.when(in_middle)
        def _():
            arrived(P_SUM, key, got.at[pl.ds(0, n - 1)])
            own[...] = jnp.sum(got[...].astype(F32), axis=0).astype(BF16)
            for p in range(1, n):
                copy_to(P_ALL, key, own, back.at[me - first_mid], lax.rem(me + p, n)).start()
            back[me - first_mid] = own[...]

    def middle_done(key, got, back):
        @pl.when(in_middle)
        def _():
            arrived(P_ALL, key, back.at[pl.ds(0, m - 1)])
            sent(P_SUM, back.at[pl.ds(0, m - 1)])
            sent(P_ALL, got.at[pl.ds(0, n - 1)])

        @pl.when(jnp.logical_not(in_middle))
        def _():
            arrived(P_ALL, key, back)
            sent(P_SUM, back)

    def level_near(key, rows_of, got):
        for p in range(1, m):
            slot = lax.rem(mine + p, m)
            copy_to(T_NEAR, key, rows_of.at[slot], got.at[mine], base + slot).start()
        got[mine] = rows_of[mine]

    def level_over(key, got, own, other):
        arrived(T_NEAR, key, got.at[pl.ds(0, m - 1)])
        own[...] = jnp.sum(got[...].astype(F32), axis=0).astype(BF16)
        copy_to(T_OVER, key, own, other, away + mine).start()

    def level_back(key, own, other, mean, back):
        arrived(T_OVER, key, other)
        mean[...] = (own[...].astype(F32) + other[...].astype(F32)).astype(BF16)
        for p in range(1, m):
            copy_to(T_BACK, key, mean, back.at[mine], base + lax.rem(mine + p, m)).start()
        back[mine] = mean[...]

    def level_sent(key_refs):
        for got, other, back in key_refs:
            sent(T_NEAR, got.at[pl.ds(0, m - 1)])
            sent(T_OVER, other)
            sent(T_BACK, back.at[pl.ds(0, m - 1)])

    for load in loads[:8]:
        load.wait()
    params = [embed[...], gain_on[...], gain_om[...], gain_in[...], gain_im[...]]
    cols[...] = jnp.concatenate(params + [jnp.zeros((2, c), F32)], axis=0).T
    here = lax.broadcasted_iota(jnp.int32, (rows, res), 1) == (
        lax.broadcasted_iota(jnp.int32, (rows, res), 0) + me * rows
    )
    row_mask = jnp.sum(jnp.where(here, residues[...], 0).astype(F32), axis=1, keepdims=True)
    row_chain = jnp.sum(jnp.where(here, chains[...], 0).astype(F32), axis=1, keepdims=True)
    both = row_mask * residues[...].astype(F32)
    same_chain = jnp.where(row_chain == chains[...].astype(F32), 1.0, 0.0)
    masks[0:1, :] = jnp.concatenate([both[i : i + 1] for i in range(rows)], axis=1)
    masks[1:2, :] = jnp.concatenate([same_chain[i : i + 1] for i in range(rows)], axis=1)
    emb0, emb1 = cols[:, 0:1], cols[:, 1:2]
    g_on, g_om, g_in, g_im = (cols[:, q : q + 1] for q in range(2, 6))
    loads[8].wait()

    def project(k):
        ds = lanes_of(k)
        same = masks[1:2, ds] > 0.5
        x = pair[ds, :].astype(F32).T + jnp.where(same, emb1, emb0)
        start[:, ds] = x
        hat, _ = norm_stats(x)
        nb = (hat * g_on).astype(BF16)
        normed[:, ds] = nb
        p = tn(out_proj[...], nb)
        pm = masks[0:1, ds]
        left = pm * sigmoid(p[:c]) * p[c : 2 * c]
        right = pm * sigmoid(p[2 * c : 3 * c]) * p[3 * c :]
        a_s[:, :, :, ds] = left.reshape(parts, m, hs, lc).astype(BF16)
        b_s[:, :, :, ds] = right.reshape(parts, m, hs, lc).astype(BF16)

    @pl.loop(0, chunks)
    def _(k):
        project(k)

    pl.semaphore_wait(barrier, n - 1)

    @pl.loop(0, parts)
    def _(h):
        near(A_OUT, h, a_s, a_r, (h,), pl.ds(0, total))
        far(B_OUT, h, b_s, b_r, (h,), pl.ds(0, total))

    for load in loads[9:]:
        load.wait()

    @pl.loop(0, chunks)
    def _(k):
        ds = lanes_of(k)
        gate[:, ds] = sigmoid(tn(out_gate[...], normed[:, ds]))
        cot_t[:, ds] = cot[ds, :].astype(F32).T

    def outgoing(h):
        arrived(A_OUT, h, a_r.at[h, pl.ds(0, m - 1)])

        @pl.loop(0, chunks)
        def _(k):
            to_slab(a_r, (h,), slab_a, h * hs, k)

        arrived(B_OUT, h, b_r.at[h, pl.ds(0, n - 1)])

        @pl.loop(0, chunks)
        def _(k):
            to_slab(b_r, (h,), slab_b, h * hs, k)

        for ch in range(hs):
            at = h * hs + ch
            keep(slab_o, at, nt(matrix(slab_a, at, half), matrix(slab_b, at, res)))

    @pl.loop(0, parts - 1)
    def _(h):
        outgoing(h)

        @pl.loop(0, chunks)
        def _(k):
            from_slab(slab_o, h * hs, x_s, (h,), k)

        near(X_OUT, h, x_s, x_r, (h,), pl.ds(0, total))

    outgoing(parts - 1)

    @pl.loop(0, chunks)
    def _(k):
        from_slab(slab_o, (parts - 1) * hs, x_s, (parts - 1,), k)
        near(X_OUT, parts - 1 + k, x_s, x_r, (parts - 1,), lanes_of(k))

    @pl.loop(0, parts - 1)
    def _(h):
        arrived(X_OUT, h, x_r.at[h, pl.ds(0, m - 1)])

    @pl.loop(0, chunks)
    def _(k):
        ds = lanes_of(k)
        arrived(X_OUT, parts - 1 + k, x_r.at[parts - 1, pl.ds(0, m - 1), :, ds])
        hat, _ = norm_stats(x_r[:, :, :, ds].astype(F32).reshape(c, lc))
        y = (hat * g_om).astype(BF16)
        v = (start[:, ds] + gate[:, ds] * tn(out_final[...], y)).astype(BF16)
        mid[:, ds] = v
        hat, _ = norm_stats(v.astype(F32))
        nb = (hat * g_in).astype(BF16)
        normed[:, ds] = nb
        p = tn(in_proj[...], nb)
        in_p[:, ds] = p
        pm = masks[0:1, ds]
        for q in range(2):
            value = pm * sigmoid(p[2 * q * c : (2 * q + 1) * c]) * p[(2 * q + 1) * c : (2 * q + 2) * c]
            put(abh_s, (q,), ds, value[every:], m, wh)
            if every:
                put(abe_s, (q,), ds, value[:every], n, we)
        near(AB_H, k, abh_s, abh_r, ALL, ds)
        if every:
            @pl.when(k > 0)
            def _():
                across(AB_E, k - 1, abe_s, abe_r, ALL, lanes_of(k - 1), True)

    if every:
        across(AB_E, chunks - 1, abe_s, abe_r, ALL, lanes_of(chunks - 1), True)

        @pl.loop(0, chunks)
        def _(k):
            across(AB_E, k, abe_s, abe_r, ALL, lanes_of(k), False)

    @pl.loop(0, chunks)
    def _(k):
        ds = lanes_of(k)
        s = sigmoid(tn(in_gate[...], normed[:, ds]))
        logit_s[:, ds] = s
        v = (cot_t[:, ds] * s).astype(BF16)
        gv[:, ds] = v
        gy[:, ds] = nn(in_final[...], v)

    acc_p[...] = jnp.zeros_like(acc_p)
    acc_g[...] = jnp.zeros_like(acc_g)
    acc_f[...] = jnp.zeros_like(acc_f)
    acc_n[...] = jnp.zeros_like(acc_n)
    acc_m[...] = jnp.zeros_like(acc_m)

    @pl.loop(0, chunks)
    def _(k):
        ds = lanes_of(k)
        arrived(AB_H, k, abh_r.at[:, pl.ds(0, m - 1), :, ds])
        to_slab(abh_r, (0,), slab_a, we, k)
        to_slab(abh_r, (1,), slab_b, we, k)

    for ch in range(wh):
        a = matrix(slab_a, we + ch, half)
        b = matrix(slab_b, we + ch, half)
        mat_a[ch] = a
        mat_b[ch] = b
        keep(slab_o, we + ch, tn(a, b))

    early_chunks = chunks - 1 if every else chunks

    @pl.loop(0, early_chunks)
    def _(k):
        from_slab(slab_o, we, xh_s, (), k)
        far(X_H, k, xh_s, xh_r, (), lanes_of(k), True)

    if every:
        from_slab(slab_o, we, xh_s, (), early_chunks)

        @pl.loop(0, chunks)
        def _(k):
            ds = lanes_of(k)
            arrived(AB_E, k, abe_r.at[:, pl.ds(0, n - 1), :, ds])
            to_slab(abe_r, (0,), slab_a, 0, k)
            to_slab(abe_r, (1,), slab_b, 0, k)

        for ch in range(we):
            a = matrix(slab_a, ch, res)
            b = matrix(slab_b, ch, res)
            mate_a[ch] = a
            mate_b[ch] = b
            keep(slab_o, ch, tn(a, b))

        def send_x(k):
            from_slab(slab_o, 0, xe_s, (), k)
            across(X_E, k, xe_s, xe_r, (), lanes_of(k), True)
            across(X_E, k, xe_s, xe_r, (), lanes_of(k), False)

        send_x(0)
        far(X_H, early_chunks, xh_s, xh_r, (), lanes_of(early_chunks), True)

        @pl.loop(1, chunks)
        def _(k):
            send_x(k)

    @pl.loop(0, chunks)
    def _(k):
        ds = lanes_of(k)
        arrived(X_H, k, xh_r.at[pl.ds(0, n - 1), :, ds])
        both = xh_r[pl.ds(0, m), :, ds].astype(F32) + xh_r[pl.ds(m, m), :, ds].astype(F32)
        x = both.reshape(c - every, lc)
        if every:
            arrived(X_E, k, xe_r.at[pl.ds(0, n - 1), :, ds])
            x = jnp.concatenate([take(xe_r, (), ds), x], axis=0)
        hat, inv = norm_stats(x)
        y = (hat * g_im).astype(BF16)
        value = tn(in_final[...], y)
        s = logit_s[:, ds]
        grad_l = (cot_t[:, ds] * value * s * (1.0 - s)).astype(BF16)
        gl[:, ds] = grad_l
        g = gy[:, ds]
        acc_m[...] += lane_sum(g * hat)
        grad_x = norm_back(g, hat, inv, g_im)
        put(gh_s, (), ds, grad_x[every:], m, wh)
        if every:
            put(ge_s, (), ds, grad_x[:every], n, we)
            across(G_E, k, ge_s, ge_r, (), ds, True)
            across(G_E, k, ge_s, ge_r, (), ds, False)
        else:
            far(G_H, k, gh_s, gh_r, (), ds)
        acc_f[...] += nt(y, gv[:, ds])

    if every:
        @pl.loop(0, chunks)
        def _(k):
            far(G_H, k, gh_s, gh_r, (), lanes_of(k))

    @pl.loop(0, chunks)
    def _(k):
        ds = lanes_of(k)
        grad_l = gl[:, ds]
        acc_g[...] += nt(normed[:, ds], grad_l)
        gy[:, ds] = nn(in_gate[...], grad_l)

    h_s[...] = early().reshape(m, c // m, 2 * c).astype(BF16)
    level_near(0, h_s, h_r)

    if every:
        @pl.loop(0, chunks)
        def _(k):
            arrived(G_E, k, ge_r.at[pl.ds(0, n - 1), :, lanes_of(k)])
            to_slab(ge_r, (), slab_a, 0, k)

        for ch in range(we):
            gx = matrix(slab_a, ch, res)
            keep(slab_o, ch, nt(mate_b[ch], gx))
            keep(slab_b, ch, nn(mate_a[ch], gx))

        @pl.loop(0, chunks)
        def _(k):
            ds = lanes_of(k)
            for q, slab in enumerate((slab_o, slab_b)):
                from_slab(slab, 0, de_s, (q,), k)
            across(D_E, k, de_s, de_r, ALL, ds, True)
            across(D_E, k, de_s, de_r, ALL, ds, False)

    @pl.loop(0, chunks)
    def _(k):
        arrived(G_H, k, gh_r.at[pl.ds(0, n - 1), :, lanes_of(k)])
        to_slab(gh_r, (), slab_a, we, k)

    for ch in range(wh):
        gx = matrix(slab_a, we + ch, res)
        keep(slab_o, we + ch, nt(mat_b[ch], gx))
        keep(slab_b, we + ch, nn(mat_a[ch], gx))

    @pl.loop(0, chunks)
    def _(k):
        for q, slab in enumerate((slab_o, slab_b)):
            from_slab(slab, we, dh_s, (q,), k)
        near(D_H, k, dh_s, dh_r, ALL, lanes_of(k))

    level_over(0, h_r, h_own, h_other)
    def finish(g, k):
        first, count = groups[g]
        ds = lanes_of(k)
        if g == 0 and every:
            arrived(D_E, k, de_r.at[:, pl.ds(0, n - 1), :, ds])
            grads = [take(de_r, (q,), ds) for q in range(2)]
        else:
            arrived(D_H, k, dh_r.at[:, pl.ds(0, m - 1), :, ds])
            grads = [take(dh_r, (q,), ds) for q in range(2)]
        pm = masks[0:1, ds]
        blocks = []
        for q in range(2):
            s = sigmoid(in_p[pl.ds(2 * q * c + first, count), ds])
            scaled = grads[q] * pm * s
            blocks.append((scaled * in_p[pl.ds((2 * q + 1) * c + first, count), ds] * (1.0 - s)).astype(BF16))
            blocks.append(scaled.astype(BF16))
        for b in range(4):
            in_q[pl.ds(b * c + first, count), ds] = blocks[b]
        acc_p[g] += nt(normed[:, ds], jnp.concatenate(blocks, axis=0))

    last = len(groups) - 1
    if every:
        @pl.loop(0, chunks)
        def _(k):
            finish(0, k)

        f_s[...] = (acc_p[0] * inv_count).reshape(m, c // m, 2 * c).astype(BF16)
        middle_sum(1, f_s, f_r)

    @pl.loop(0, chunks)
    def _(k):
        finish(last, k)

    g_s[...] = (acc_p[last] * inv_count).reshape(m, c // m, 4 * groups[last][1]).astype(BF16)
    middle_sum(0, g_s, g_r)
    level_back(0, h_own, h_other, h_mean, h_back)

    @pl.loop(0, chunks)
    def _(k):
        ds = lanes_of(k)
        g = nn(in_proj[...], in_q[:, ds]) + gy[:, ds]
        hat, inv = norm_stats(mid[:, ds].astype(F32))
        acc_n[...] += lane_sum(g * hat)
        z = cot_t[:, ds] + norm_back(g, hat, inv, g_in)
        grad_out[ds, :] = z.T.astype(BF16)

    lane = lax.broadcasted_iota(jnp.int32, (c, LANES), 1)
    gains = jnp.where(lane == 0, acc_n[...], jnp.where(lane == 1, acc_m[...], 0.0))
    w_s[...] = (gains * inv_count).T[:2]
    for p in range(1, n):
        copy_to(GAINS, 0, w_s, w_r.at[me], lax.rem(me + p, n)).start()
    w_r[me] = w_s[...]
    if every:
        middle_round(1, f_r, f_own, f_back)
    middle_round(0, g_r, t_s, t_r)
    arrived(T_BACK, 0, h_back.at[pl.ds(0, m - 1)])
    both = h_back[...].astype(F32).reshape(c, 2 * c)
    gg_out[...] = both[:, :c]
    gf_out[...] = both[:, c:]
    arrived(GAINS, 0, w_r.at[pl.ds(0, n - 1)])
    gain_sums = jnp.sum(w_r[...], axis=0)
    gn_out[...] = gain_sums[0:1]
    gm_out[...] = gain_sums[1:2]

    for h in range(parts):
        sent(A_OUT, a_r.at[h, pl.ds(0, m - 1)])
        sent(B_OUT, b_r.at[h, pl.ds(0, n - 1)])
        sent(X_OUT, x_r.at[h, pl.ds(0, m - 1)])
    for q in range(2):
        sent(AB_H, abh_r.at[q, pl.ds(0, m - 1)])
        sent(D_H, dh_r.at[q, pl.ds(0, m - 1)])
    sent(X_H, xh_r.at[pl.ds(0, n - 1)])
    sent(G_H, gh_r.at[pl.ds(0, n - 1)])
    if every:
        for q in range(2):
            sent(AB_E, abe_r.at[q, pl.ds(0, n - 1)])
            sent(D_E, de_r.at[q, pl.ds(0, n - 1)])
        sent(X_E, xe_r.at[pl.ds(0, n - 1)])
        sent(G_E, ge_r.at[pl.ds(0, n - 1)])
    sent(GAINS, w_r.at[pl.ds(0, n - 1)])
    level_sent([(h_r, h_other, h_back)])

    for g, (first, count) in enumerate(groups):
        if g == 0 and every:
            middle_done(1, f_r, f_back)
            whole = f_back[...].astype(F32).reshape(c, 4 * count)
        else:
            middle_done(0, g_r, t_r)
            whole = t_r[...].astype(F32).reshape(c, 4 * count)
        for b in range(4):
            gp_out[:, b * c + first : b * c + first + count] = whole[:, b * count : (b + 1) * count]


def write_out(*refs):
    sems = refs[-1]
    copies = [pltpu.make_async_copy(refs[q], refs[q + 6], sems.at[q]) for q in range(6)]
    for copy in copies:
        copy.start()
    for copy in copies:
        copy.wait()


def shards(n, pair, cotangent, residue_mask, chain_ids, chain_embed, out_norm_gain, out_proj,
           out_gate, out_mid_gain, out_final, in_norm_gain, in_proj, in_gate, in_mid_gain, in_final):
    rows, res, c = pair.shape
    total = rows * res
    per = c // n
    lc = res * min(
        q for q in range(1, rows + 1)
        if rows % q == 0 and q * res % LANES == 0 and (rows // q <= 3)
    )
    tiles = -(-res // LANES)
    def full(dtype):
        return pltpu.VMEM((c, total), dtype)

    def block(*shape):
        return pltpu.VMEM((*shape, total), BF16)

    m = n // 2
    hc = c // m
    parts = hc // 8 if hc % 8 == 0 else 1
    every = c // 2 if (c // 2) % (8 * n) == 0 else 0
    we, wh = max(every // n, 8), (c - every) // m
    groups = 2 if every else 1
    wide = 4 * c // groups
    pitch = max(hc, every // n + wh) + PAD
    hs = hc // parts
    chunks = total // lc
    slab = pltpu.VMEM((tiles, res * pitch, LANES), F32)
    small = n if every else 1
    scratch = [
        pltpu.VMEM((total, c), BF16), pltpu.VMEM((total, c), BF16), pltpu.VMEM((1, res), jnp.int32), pltpu.VMEM((1, res), jnp.int32),
        pltpu.VMEM((2, c), F32),
    ] + [pltpu.VMEM((1, c), F32)] * 4 + [
        pltpu.VMEM((c, 4 * c), BF16), pltpu.VMEM((c, c), BF16), pltpu.VMEM((c, c), BF16),
        pltpu.VMEM((c, 4 * c), BF16), pltpu.VMEM((c, c), BF16), pltpu.VMEM((c, c), BF16),
        pltpu.VMEM((c, 8), F32), pltpu.VMEM((2, total), F32), pltpu.VMEM((4 * c, total), BF16), full(F32), full(BF16), full(F32),
        pltpu.VMEM((4 * c, total), F32), full(F32), full(BF16), full(F32), full(BF16), full(F32), full(BF16),
        block(parts, m, hs), block(parts, m, hs), block(parts, m, hs),
        block(parts, m, hs), block(parts, n, hs), block(parts, m, hs),
        block(2, m, wh), block(2, m, wh), block(n, wh), block(n, wh),
        block(m, wh), block(n, wh), block(2, m, wh), block(2, m, wh),
        block(2, small, we), block(2, small, we), block(small, we), block(small, we),
        block(small, we), block(small, we), block(2, small, we), block(2, small, we),
        slab, slab, slab,
        pltpu.VMEM((wh, m * rows, res), BF16), pltpu.VMEM((wh, m * rows, res), BF16),
        pltpu.VMEM((we, res, res), BF16), pltpu.VMEM((we, res, res), BF16),
        pltpu.VMEM((groups, c, wide), F32), pltpu.VMEM((c, c), F32), pltpu.VMEM((c, c), F32),
        pltpu.VMEM((c, 1), F32), pltpu.VMEM((c, 1), F32),
        pltpu.VMEM((m, hc, wide), BF16), pltpu.VMEM((n, hc, wide), BF16),
        pltpu.VMEM((hc, wide), BF16), pltpu.VMEM((m, hc, wide), BF16),
    ] + [
        pltpu.VMEM(shape, BF16)
        for shape in ((m, hc, 2 * c), (m, hc, 2 * c), (hc, 2 * c), (hc, 2 * c), (hc, 2 * c), (m, hc, 2 * c))
    ] + [
        pltpu.VMEM(shape, BF16) for shape in ((m, hc, wide), (n, hc, wide), (hc, wide), (m, hc, wide))
    ] + [
        pltpu.VMEM((2, c), F32), pltpu.VMEM((n, 2, c), F32),
        pltpu.SemaphoreType.DMA((15,)), pltpu.SemaphoreType.DMA((17,)), pltpu.SemaphoreType.DMA((receive_slots(parts, chunks)[-1],)),
    ]
    vmem = pl.BlockSpec(memory_space=pltpu.VMEM)
    results = pl.pallas_call(
        functools.partial(kernel, n, rows, res, lc, pitch, every),
        out_shape=(
            pltpu.VMEM((total, c), BF16),
            pltpu.VMEM((c, 4 * c), F32),
            pltpu.VMEM((c, c), F32),
            pltpu.VMEM((c, c), F32),
            pltpu.VMEM((1, c), F32),
            pltpu.VMEM((1, c), F32),
        ),
        in_specs=[pl.BlockSpec(memory_space=pl.ANY)] * 15,
        out_specs=(vmem,) * 6,
        scratch_shapes=scratch,
        compiler_params=pltpu.CompilerParams(
            collective_id=0, has_side_effects=True, vmem_limit_bytes=56 * 1024 * 1024
        ),
    )(
        pair.reshape(total, c), cotangent.reshape(total, c),
        residue_mask.reshape(1, res), chain_ids.reshape(1, res), chain_embed,
        out_norm_gain.reshape(1, c), out_mid_gain.reshape(1, c),
        in_norm_gain.reshape(1, c), in_mid_gain.reshape(1, c),
        out_proj, out_gate, out_final, in_proj, in_gate, in_final,
    )
    shapes = [((total, c), BF16), ((c, 4 * c), F32), ((c, c), F32), ((c, c), F32), ((1, c), F32), ((1, c), F32)]
    grad, gp, gg, gf, gn, gm = pl.pallas_call(
        write_out,
        out_shape=[jax.ShapeDtypeStruct(*shape) for shape in shapes],
        in_specs=[pl.BlockSpec(memory_space=pltpu.VMEM)] * 6,
        out_specs=[pl.BlockSpec(memory_space=pl.ANY)] * 6,
        scratch_shapes=[pltpu.SemaphoreType.DMA((6,))],
    )(*[pltpu.with_memory_space_constraint(r, pltpu.VMEM) for r in results])
    return grad.reshape(rows, res, c), gp, gg, gf, gn.reshape(c), gm.reshape(c)


def solution(mesh):
    split = P("dap", "cplx", None)
    return jax.shard_map(
        functools.partial(shards, mesh.shape["dap"]),
        mesh=mesh,
        in_specs=(split, split, P("cplx"), P("cplx")) + (P(),) * 11,
        out_specs=(split, P("cplx", None), P("cplx", None), P("cplx", None), P("cplx"), P("cplx")),
        check_vma=False,
    )
```

```python
import functools

import jax
import jax.numpy as jnp
from jax import lax
from jax.experimental import pallas as pl
from jax.experimental.pallas import tpu as pltpu
from jax.sharding import PartitionSpec as P

F32 = jnp.float32
BF16 = jnp.bfloat16
LANES = 128
PAD = 8
ALL = (slice(None),)
A_OUT, B_OUT, X_OUT, AB_H, X_H, G_H, D_H, AB_E, X_E, G_E, D_E, GAINS, P_SUM, P_ALL, T_NEAR, T_OVER, T_BACK = range(17)


def tn(w, x):
    return lax.dot_general(w, x, (((0,), (0,)), ((), ())), preferred_element_type=F32)


def nn(w, x):
    return jnp.dot(w, x, preferred_element_type=F32)


def nt(w, x):
    return lax.dot_general(w, x, (((1,), (1,)), ((), ())), preferred_element_type=F32)


def sigmoid(v):
    return 1.0 / (1.0 + jnp.exp(-v))


def norm_stats(v):
    centred = v - jnp.mean(v, axis=0, keepdims=True)
    inv = lax.rsqrt(jnp.mean(centred * centred, axis=0, keepdims=True) + 1e-05)
    return centred * inv, inv


def norm_back(grad, hat, inv, gain):
    scaled = grad * gain
    m1 = jnp.mean(scaled, axis=0, keepdims=True)
    m2 = jnp.mean(scaled * hat, axis=0, keepdims=True)
    return inv * (scaled - m1 - hat * m2)


def lane_sum(v):
    return jnp.sum(v, axis=1, keepdims=True)


def receive_slots(parts, chunks):
    counts = [parts, parts, parts - 1 + chunks] + [chunks] * 8 + [1, 2, 2, 1, 1, 1]
    return [sum(counts[:q]) for q in range(len(counts) + 1)]


def kernel(
    n, rows, res, lc, pitch, every,
    pair_h, cot_h, residues_h, chains_h, embed_h, gain_on_h, gain_om_h, gain_in_h, gain_im_h,
    out_proj_h, out_gate_h, out_final_h, in_proj_h, in_gate_h, in_final_h,
    grad_out, gp_out, gg_out, gf_out, gn_out, gm_out,
    pair, cot, residues, chains, embed, gain_on, gain_om, gain_in, gain_im,
    out_proj, out_gate, out_final, in_proj, in_gate, in_final,
    cols, masks, in_q, start, normed, gate, in_p, cot_t, mid, logit_s, gv, gy, gl,
    a_s, b_s, x_s, a_r, b_r, x_r,
    abh_s, abh_r, xh_s, xh_r, gh_s, gh_r, dh_s, dh_r,
    abe_s, abe_r, xe_s, xe_r, ge_s, ge_r, de_s, de_r,
    slab_a, slab_b, slab_o, mat_a, mat_b, mate_a, mate_b,
    acc_p, acc_g, acc_f, acc_n, acc_m, g_s, g_r, t_s, t_r,
    h_s, h_r, h_own, h_other, h_mean, h_back, f_s, f_r, f_own, f_back, w_s, w_r,
    in_sem, send_sem, recv_sem,
):
    me = lax.axis_index("dap")
    c = start.shape[0]
    per = c // n
    m = n // 2
    parts, hs = a_s.shape[0], a_s.shape[2]
    mine = lax.rem(me, m)
    base = me - mine
    away = m - base
    half = m * rows
    total = rows * res
    chunks = total // lc
    crows = lc // res
    tiles = -(-res // LANES)
    inv_count = 1.0 / res
    we, wh = every // n, (c - every) // m
    groups = ([(0, every)] if every else []) + [(every, c - every)]

    barrier = pltpu.get_barrier_semaphore()
    for p in range(1, n):
        pl.semaphore_signal(
            barrier, inc=1, device_id={"dap": lax.rem(me + p, n)},
            device_id_type=pl.DeviceIdType.MESH,
        )
    sources = [
        pair_h, embed_h, gain_on_h, gain_om_h, gain_in_h, gain_im_h, residues_h, chains_h, out_proj_h,
        out_gate_h, cot_h, out_final_h, in_proj_h, in_gate_h, in_final_h,
    ]
    targets = [
        pair, embed, gain_on, gain_om, gain_in, gain_im, residues, chains, out_proj,
        out_gate, cot, out_final, in_proj, in_gate, in_final,
    ]
    loads = [pltpu.make_async_copy(a, b, in_sem.at[q]) for q, (a, b) in enumerate(zip(sources, targets))]
    for load in loads:
        load.start()

    first_of = receive_slots(parts, chunks)

    def copy_to(which, k, src, dst, peer):
        return pltpu.make_async_remote_copy(
            src_ref=src, dst_ref=dst, send_sem=send_sem.at[which], recv_sem=recv_sem.at[first_of[which] + k],
            device_id={"dap": peer}, device_id_type=pl.DeviceIdType.MESH,
        )

    def lanes_of(k):
        return pl.ds(pl.multiple_of(k * lc, lc), lc)

    def near(which, key, src, dst, lead, ds):
        for p in range(1, m):
            slot = lax.rem(mine + p, m)
            copy_to(which, key, src.at[(*lead, slot, slice(None), ds)], dst.at[(*lead, mine, slice(None), ds)], base + slot).start()
        dst[(*lead, mine, slice(None), ds)] = src[(*lead, mine, slice(None), ds)]

    def far(which, key, src, dst, lead, ds, by_peer=False):
        for first, other in ((0, True), (1, False)):
            for p in range(first, m):
                slot = lax.rem(mine + p, m)
                peer = (away if other else base) + slot
                at = peer if by_peer else slot
                copy_to(which, key, src.at[(*lead, at, slice(None), ds)], dst.at[(*lead, me, slice(None), ds)], peer).start()
        dst[(*lead, me, slice(None), ds)] = src[(*lead, me if by_peer else mine, slice(None), ds)]

    def across(which, key, src, dst, lead, ds, other):
        for p in range(0 if other else 1, m):
            peer = (away if other else base) + lax.rem(mine + p, m)
            copy_to(which, key, src.at[(*lead, peer, slice(None), ds)], dst.at[(*lead, me, slice(None), ds)], peer).start()
        if not other:
            dst[(*lead, me, slice(None), ds)] = src[(*lead, me, slice(None), ds)]

    def arrived(which, key, block):
        copy_to(which, key, block, block, lax.rem(me + 1, n)).wait_recv()

    def sent(which, block):
        copy_to(which, 0, block, block, lax.rem(me + 1, n)).wait_send()

    def put(ref, lead, ds, value, count, width):
        ref[(*lead, slice(None), slice(None), ds)] = value.reshape(count, width, lc).astype(BF16)

    def take(ref, lead, ds):
        block = ref[(*lead, slice(None), slice(None), ds)].astype(F32)
        return block.reshape(block.shape[0] * block.shape[1], lc)

    def to_slab(ref, lead, slab, slot, k):
        ds = lanes_of(k)
        width_c = ref.shape[-2]
        for s in range(ref.shape[-3]):
            block = ref[(*lead, s, slice(None), ds)].astype(F32)
            row = s * rows + k * crows
            for i in range(crows):
                part = block[:, i * res : (i + 1) * res]
                at = pl.ds(pl.multiple_of((row + i) * pitch + slot, 8), width_c)
                for t in range(tiles):
                    width = min(LANES, res - t * LANES)
                    slab[t, at, :width] = part[:, t * LANES : t * LANES + width]

    def matrix(slab, ch, count):
        at = pl.ds(ch, count, stride=pitch)
        pieces = [slab[t, at, :] for t in range(tiles)]
        whole = pieces[0] if tiles == 1 else jnp.concatenate(pieces, axis=1)
        return whole[:, :res].astype(BF16)

    def keep(slab, ch, value):
        count = value.shape[0]
        pad = tiles * LANES - res
        if pad:
            value = jnp.concatenate([value, jnp.zeros((count, pad), F32)], axis=1)
        for t in range(tiles):
            slab[t, pl.ds(ch, count, stride=pitch), :] = value[:, t * LANES : (t + 1) * LANES]

    def from_slab(slab, slot, ref, lead, k):
        width_c = ref.shape[-2]
        for s in range(ref.shape[-3]):
            row = s * rows + k * crows
            pieces = []
            for i in range(crows):
                at = pl.ds(pl.multiple_of((row + i) * pitch + slot, 8), width_c)
                for t in range(tiles):
                    width = min(LANES, res - t * LANES)
                    pieces.append(slab[t, at, :width])
            ref[(*lead, s, slice(None), lanes_of(k))] = jnp.concatenate(pieces, axis=1).astype(BF16)

    def early():
        return jnp.concatenate([acc_g[...], acc_f[...]], axis=1) * inv_count

    first_mid = n // 4
    in_middle = (me >= first_mid) & (me < first_mid + m)

    def middle_sum(key, src, got):
        for r in range(m):
            @pl.when(me != first_mid + r)
            def _():
                copy_to(P_SUM, key, src.at[r], got.at[me], first_mid + r).start()

        @pl.when(in_middle)
        def _():
            got[me] = src[me - first_mid]

    def middle_round(key, got, own, back):
        @pl.when(in_middle)
        def _():
            arrived(P_SUM, key, got.at[pl.ds(0, n - 1)])
            own[...] = jnp.sum(got[...].astype(F32), axis=0).astype(BF16)
            for p in range(1, n):
                copy_to(P_ALL, key, own, back.at[me - first_mid], lax.rem(me + p, n)).start()
            back[me - first_mid] = own[...]

    def middle_done(key, got, back):
        @pl.when(in_middle)
        def _():
            arrived(P_ALL, key, back.at[pl.ds(0, m - 1)])
            sent(P_SUM, back.at[pl.ds(0, m - 1)])
            sent(P_ALL, got.at[pl.ds(0, n - 1)])

        @pl.when(jnp.logical_not(in_middle))
        def _():
            arrived(P_ALL, key, back)
            sent(P_SUM, back)

    def level_near(key, rows_of, got):
        for p in range(1, m):
            slot = lax.rem(mine + p, m)
            copy_to(T_NEAR, key, rows_of.at[slot], got.at[mine], base + slot).start()
        got[mine] = rows_of[mine]

    def level_over(key, got, own, other):
        arrived(T_NEAR, key, got.at[pl.ds(0, m - 1)])
        own[...] = jnp.sum(got[...].astype(F32), axis=0).astype(BF16)
        copy_to(T_OVER, key, own, other, away + mine).start()

    def level_back(key, own, other, mean, back):
        arrived(T_OVER, key, other)
        mean[...] = (own[...].astype(F32) + other[...].astype(F32)).astype(BF16)
        for p in range(1, m):
            copy_to(T_BACK, key, mean, back.at[mine], base + lax.rem(mine + p, m)).start()
        back[mine] = mean[...]

    def level_sent(key_refs):
        for got, other, back in key_refs:
            sent(T_NEAR, got.at[pl.ds(0, m - 1)])
            sent(T_OVER, other)
            sent(T_BACK, back.at[pl.ds(0, m - 1)])

    for load in loads[:8]:
        load.wait()
    params = [embed[...], gain_on[...], gain_om[...], gain_in[...], gain_im[...]]
    cols[...] = jnp.concatenate(params + [jnp.zeros((2, c), F32)], axis=0).T
    here = lax.broadcasted_iota(jnp.int32, (rows, res), 1) == (
        lax.broadcasted_iota(jnp.int32, (rows, res), 0) + me * rows
    )
    row_mask = jnp.sum(jnp.where(here, residues[...], 0).astype(F32), axis=1, keepdims=True)
    row_chain = jnp.sum(jnp.where(here, chains[...], 0).astype(F32), axis=1, keepdims=True)
    both = row_mask * residues[...].astype(F32)
    same_chain = jnp.where(row_chain == chains[...].astype(F32), 1.0, 0.0)
    masks[0:1, :] = jnp.concatenate([both[i : i + 1] for i in range(rows)], axis=1)
    masks[1:2, :] = jnp.concatenate([same_chain[i : i + 1] for i in range(rows)], axis=1)
    emb0, emb1 = cols[:, 0:1], cols[:, 1:2]
    g_on, g_om, g_in, g_im = (cols[:, q : q + 1] for q in range(2, 6))
    loads[8].wait()

    def project(k):
        ds = lanes_of(k)
        same = masks[1:2, ds] > 0.5
        x = pair[ds, :].astype(F32).T + jnp.where(same, emb1, emb0)
        start[:, ds] = x
        hat, _ = norm_stats(x)
        nb = (hat * g_on).astype(BF16)
        normed[:, ds] = nb
        p = tn(out_proj[...], nb)
        pm = masks[0:1, ds]
        left = pm * sigmoid(p[:c]) * p[c : 2 * c]
        right = pm * sigmoid(p[2 * c : 3 * c]) * p[3 * c :]
        a_s[:, :, :, ds] = left.reshape(parts, m, hs, lc).astype(BF16)
        b_s[:, :, :, ds] = right.reshape(parts, m, hs, lc).astype(BF16)

    @pl.loop(0, chunks)
    def _(k):
        project(k)

    pl.semaphore_wait(barrier, n - 1)

    @pl.loop(0, parts)
    def _(h):
        near(A_OUT, h, a_s, a_r, (h,), pl.ds(0, total))
        far(B_OUT, h, b_s, b_r, (h,), pl.ds(0, total))

    for load in loads[9:]:
        load.wait()

    @pl.loop(0, chunks)
    def _(k):
        ds = lanes_of(k)
        gate[:, ds] = sigmoid(tn(out_gate[...], normed[:, ds]))
        cot_t[:, ds] = cot[ds, :].astype(F32).T

    def outgoing(h):
        arrived(A_OUT, h, a_r.at[h, pl.ds(0, m - 1)])

        @pl.loop(0, chunks)
        def _(k):
            to_slab(a_r, (h,), slab_a, h * hs, k)

        arrived(B_OUT, h, b_r.at[h, pl.ds(0, n - 1)])

        @pl.loop(0, chunks)
        def _(k):
            to_slab(b_r, (h,), slab_b, h * hs, k)

        for ch in range(hs):
            at = h * hs + ch
            keep(slab_o, at, nt(matrix(slab_a, at, half), matrix(slab_b, at, res)))

    @pl.loop(0, parts - 1)
    def _(h):
        outgoing(h)

        @pl.loop(0, chunks)
        def _(k):
            from_slab(slab_o, h * hs, x_s, (h,), k)

        near(X_OUT, h, x_s, x_r, (h,), pl.ds(0, total))

    outgoing(parts - 1)

    @pl.loop(0, chunks)
    def _(k):
        from_slab(slab_o, (parts - 1) * hs, x_s, (parts - 1,), k)
        near(X_OUT, parts - 1 + k, x_s, x_r, (parts - 1,), lanes_of(k))

    @pl.loop(0, parts - 1)
    def _(h):
        arrived(X_OUT, h, x_r.at[h, pl.ds(0, m - 1)])

    @pl.loop(0, chunks)
    def _(k):
        ds = lanes_of(k)
        arrived(X_OUT, parts - 1 + k, x_r.at[parts - 1, pl.ds(0, m - 1), :, ds])
        hat, _ = norm_stats(x_r[:, :, :, ds].astype(F32).reshape(c, lc))
        y = (hat * g_om).astype(BF16)
        v = (start[:, ds] + gate[:, ds] * tn(out_final[...], y)).astype(BF16)
        mid[:, ds] = v
        hat, _ = norm_stats(v.astype(F32))
        nb = (hat * g_in).astype(BF16)
        normed[:, ds] = nb
        p = tn(in_proj[...], nb)
        in_p[:, ds] = p
        pm = masks[0:1, ds]
        for q in range(2):
            value = pm * sigmoid(p[2 * q * c : (2 * q + 1) * c]) * p[(2 * q + 1) * c : (2 * q + 2) * c]
            put(abh_s, (q,), ds, value[every:], m, wh)
            if every:
                put(abe_s, (q,), ds, value[:every], n, we)
        near(AB_H, k, abh_s, abh_r, ALL, ds)
        if every:
            pass

    if every:
        @pl.loop(0, chunks)
        def _(k):
            across(AB_E, k, abe_s, abe_r, ALL, lanes_of(k), True)

        @pl.loop(0, chunks)
        def _(k):
            across(AB_E, k, abe_s, abe_r, ALL, lanes_of(k), False)

    @pl.loop(0, chunks)
    def _(k):
        ds = lanes_of(k)
        s = sigmoid(tn(in_gate[...], normed[:, ds]))
        logit_s[:, ds] = s
        v = (cot_t[:, ds] * s).astype(BF16)
        gv[:, ds] = v
        gy[:, ds] = nn(in_final[...], v)

    acc_p[...] = jnp.zeros_like(acc_p)
    acc_g[...] = jnp.zeros_like(acc_g)
    acc_f[...] = jnp.zeros_like(acc_f)
    acc_n[...] = jnp.zeros_like(acc_n)
    acc_m[...] = jnp.zeros_like(acc_m)

    @pl.loop(0, chunks)
    def _(k):
        ds = lanes_of(k)
        arrived(AB_H, k, abh_r.at[:, pl.ds(0, m - 1), :, ds])
        to_slab(abh_r, (0,), slab_a, we, k)
        to_slab(abh_r, (1,), slab_b, we, k)

    for ch in range(wh):
        a = matrix(slab_a, we + ch, half)
        b = matrix(slab_b, we + ch, half)
        mat_a[ch] = a
        mat_b[ch] = b
        keep(slab_o, we + ch, tn(a, b))

    early_chunks = chunks - 1 if every else chunks

    @pl.loop(0, early_chunks)
    def _(k):
        from_slab(slab_o, we, xh_s, (), k)
        far(X_H, k, xh_s, xh_r, (), lanes_of(k), True)

    if every:
        from_slab(slab_o, we, xh_s, (), early_chunks)

        @pl.loop(0, chunks)
        def _(k):
            ds = lanes_of(k)
            arrived(AB_E, k, abe_r.at[:, pl.ds(0, n - 1), :, ds])
            to_slab(abe_r, (0,), slab_a, 0, k)
            to_slab(abe_r, (1,), slab_b, 0, k)

        for ch in range(we):
            a = matrix(slab_a, ch, res)
            b = matrix(slab_b, ch, res)
            mate_a[ch] = a
            mate_b[ch] = b
            keep(slab_o, ch, tn(a, b))

        def send_x(k):
            from_slab(slab_o, 0, xe_s, (), k)
            across(X_E, k, xe_s, xe_r, (), lanes_of(k), True)
            across(X_E, k, xe_s, xe_r, (), lanes_of(k), False)

        send_x(0)
        far(X_H, early_chunks, xh_s, xh_r, (), lanes_of(early_chunks), True)

        @pl.loop(1, chunks)
        def _(k):
            send_x(k)

    @pl.loop(0, chunks)
    def _(k):
        ds = lanes_of(k)
        arrived(X_H, k, xh_r.at[pl.ds(0, n - 1), :, ds])
        both = xh_r[pl.ds(0, m), :, ds].astype(F32) + xh_r[pl.ds(m, m), :, ds].astype(F32)
        x = both.reshape(c - every, lc)
        if every:
            arrived(X_E, k, xe_r.at[pl.ds(0, n - 1), :, ds])
            x = jnp.concatenate([take(xe_r, (), ds), x], axis=0)
        hat, inv = norm_stats(x)
        y = (hat * g_im).astype(BF16)
        value = tn(in_final[...], y)
        s = logit_s[:, ds]
        grad_l = (cot_t[:, ds] * value * s * (1.0 - s)).astype(BF16)
        gl[:, ds] = grad_l
        g = gy[:, ds]
        acc_m[...] += lane_sum(g * hat)
        grad_x = norm_back(g, hat, inv, g_im)
        put(gh_s, (), ds, grad_x[every:], m, wh)
        if every:
            put(ge_s, (), ds, grad_x[:every], n, we)
            across(G_E, k, ge_s, ge_r, (), ds, True)
        else:
            far(G_H, k, gh_s, gh_r, (), ds)
        acc_f[...] += nt(y, gv[:, ds])

    if every:
        @pl.loop(0, chunks)
        def _(k):
            across(G_E, k, ge_s, ge_r, (), lanes_of(k), False)

        @pl.loop(0, chunks)
        def _(k):
            far(G_H, k, gh_s, gh_r, (), lanes_of(k))

    @pl.loop(0, chunks)
    def _(k):
        ds = lanes_of(k)
        grad_l = gl[:, ds]
        acc_g[...] += nt(normed[:, ds], grad_l)
        gy[:, ds] = nn(in_gate[...], grad_l)

    h_s[...] = early().reshape(m, c // m, 2 * c).astype(BF16)
    level_near(0, h_s, h_r)

    if every:
        @pl.loop(0, chunks)
        def _(k):
            arrived(G_E, k, ge_r.at[pl.ds(0, n - 1), :, lanes_of(k)])
            to_slab(ge_r, (), slab_a, 0, k)

        for ch in range(we):
            gx = matrix(slab_a, ch, res)
            keep(slab_o, ch, nt(mate_b[ch], gx))
            keep(slab_b, ch, nn(mate_a[ch], gx))

        @pl.loop(0, chunks)
        def _(k):
            ds = lanes_of(k)
            for q, slab in enumerate((slab_o, slab_b)):
                from_slab(slab, 0, de_s, (q,), k)
            across(D_E, k, de_s, de_r, ALL, ds, True)
            across(D_E, k, de_s, de_r, ALL, ds, False)

    @pl.loop(0, chunks)
    def _(k):
        arrived(G_H, k, gh_r.at[pl.ds(0, n - 1), :, lanes_of(k)])
        to_slab(gh_r, (), slab_a, we, k)

    for ch in range(wh):
        gx = matrix(slab_a, we + ch, res)
        keep(slab_o, we + ch, nt(mat_b[ch], gx))
        keep(slab_b, we + ch, nn(mat_a[ch], gx))

    @pl.loop(0, chunks)
    def _(k):
        for q, slab in enumerate((slab_o, slab_b)):
            from_slab(slab, we, dh_s, (q,), k)
        near(D_H, k, dh_s, dh_r, ALL, lanes_of(k))

    level_over(0, h_r, h_own, h_other)
    def finish(g, k):
        first, count = groups[g]
        ds = lanes_of(k)
        if g == 0 and every:
            arrived(D_E, k, de_r.at[:, pl.ds(0, n - 1), :, ds])
            grads = [take(de_r, (q,), ds) for q in range(2)]
        else:
            arrived(D_H, k, dh_r.at[:, pl.ds(0, m - 1), :, ds])
            grads = [take(dh_r, (q,), ds) for q in range(2)]
        pm = masks[0:1, ds]
        blocks = []
        for q in range(2):
            s = sigmoid(in_p[pl.ds(2 * q * c + first, count), ds])
            scaled = grads[q] * pm * s
            blocks.append((scaled * in_p[pl.ds((2 * q + 1) * c + first, count), ds] * (1.0 - s)).astype(BF16))
            blocks.append(scaled.astype(BF16))
        for b in range(4):
            in_q[pl.ds(b * c + first, count), ds] = blocks[b]
        acc_p[g] += nt(normed[:, ds], jnp.concatenate(blocks, axis=0))

    last = len(groups) - 1
    if every:
        @pl.loop(0, chunks)
        def _(k):
            finish(0, k)

        f_s[...] = (acc_p[0] * inv_count).reshape(m, c // m, 2 * c).astype(BF16)
        middle_sum(1, f_s, f_r)

    @pl.loop(0, chunks)
    def _(k):
        finish(last, k)

    g_s[...] = (acc_p[last] * inv_count).reshape(m, c // m, 4 * groups[last][1]).astype(BF16)
    middle_sum(0, g_s, g_r)
    level_back(0, h_own, h_other, h_mean, h_back)

    @pl.loop(0, chunks)
    def _(k):
        ds = lanes_of(k)
        g = nn(in_proj[...], in_q[:, ds]) + gy[:, ds]
        hat, inv = norm_stats(mid[:, ds].astype(F32))
        acc_n[...] += lane_sum(g * hat)
        z = cot_t[:, ds] + norm_back(g, hat, inv, g_in)
        grad_out[ds, :] = z.T.astype(BF16)

    lane = lax.broadcasted_iota(jnp.int32, (c, LANES), 1)
    gains = jnp.where(lane == 0, acc_n[...], jnp.where(lane == 1, acc_m[...], 0.0))
    w_s[...] = (gains * inv_count).T[:2]
    for p in range(1, n):
        copy_to(GAINS, 0, w_s, w_r.at[me], lax.rem(me + p, n)).start()
    w_r[me] = w_s[...]
    if every:
        middle_round(1, f_r, f_own, f_back)
    middle_round(0, g_r, t_s, t_r)
    arrived(T_BACK, 0, h_back.at[pl.ds(0, m - 1)])
    both = h_back[...].astype(F32).reshape(c, 2 * c)
    gg_out[...] = both[:, :c]
    gf_out[...] = both[:, c:]
    arrived(GAINS, 0, w_r.at[pl.ds(0, n - 1)])
    gain_sums = jnp.sum(w_r[...], axis=0)
    gn_out[...] = gain_sums[0:1]
    gm_out[...] = gain_sums[1:2]

    for h in range(parts):
        sent(A_OUT, a_r.at[h, pl.ds(0, m - 1)])
        sent(B_OUT, b_r.at[h, pl.ds(0, n - 1)])
        sent(X_OUT, x_r.at[h, pl.ds(0, m - 1)])
    for q in range(2):
        sent(AB_H, abh_r.at[q, pl.ds(0, m - 1)])
        sent(D_H, dh_r.at[q, pl.ds(0, m - 1)])
    sent(X_H, xh_r.at[pl.ds(0, n - 1)])
    sent(G_H, gh_r.at[pl.ds(0, n - 1)])
    if every:
        for q in range(2):
            sent(AB_E, abe_r.at[q, pl.ds(0, n - 1)])
            sent(D_E, de_r.at[q, pl.ds(0, n - 1)])
        sent(X_E, xe_r.at[pl.ds(0, n - 1)])
        sent(G_E, ge_r.at[pl.ds(0, n - 1)])
    sent(GAINS, w_r.at[pl.ds(0, n - 1)])
    level_sent([(h_r, h_other, h_back)])

    for g, (first, count) in enumerate(groups):
        if g == 0 and every:
            middle_done(1, f_r, f_back)
            whole = f_back[...].astype(F32).reshape(c, 4 * count)
        else:
            middle_done(0, g_r, t_r)
            whole = t_r[...].astype(F32).reshape(c, 4 * count)
        for b in range(4):
            gp_out[:, b * c + first : b * c + first + count] = whole[:, b * count : (b + 1) * count]


def write_out(*refs):
    sems = refs[-1]
    copies = [pltpu.make_async_copy(refs[q], refs[q + 6], sems.at[q]) for q in range(6)]
    for copy in copies:
        copy.start()
    for copy in copies:
        copy.wait()


def shards(n, pair, cotangent, residue_mask, chain_ids, chain_embed, out_norm_gain, out_proj,
           out_gate, out_mid_gain, out_final, in_norm_gain, in_proj, in_gate, in_mid_gain, in_final):
    rows, res, c = pair.shape
    total = rows * res
    per = c // n
    lc = res * min(
        q for q in range(1, rows + 1)
        if rows % q == 0 and q * res % LANES == 0 and (rows // q <= 3)
    )
    tiles = -(-res // LANES)
    def full(dtype):
        return pltpu.VMEM((c, total), dtype)

    def block(*shape):
        return pltpu.VMEM((*shape, total), BF16)

    m = n // 2
    hc = c // m
    parts = hc // 8 if hc % 8 == 0 else 1
    every = c // 2 if (c // 2) % (8 * n) == 0 else 0
    we, wh = max(every // n, 8), (c - every) // m
    groups = 2 if every else 1
    wide = 4 * c // groups
    pitch = max(hc, every // n + wh) + PAD
    hs = hc // parts
    chunks = total // lc
    slab = pltpu.VMEM((tiles, res * pitch, LANES), F32)
    small = n if every else 1
    scratch = [
        pltpu.VMEM((total, c), BF16), pltpu.VMEM((total, c), BF16), pltpu.VMEM((1, res), jnp.int32), pltpu.VMEM((1, res), jnp.int32),
        pltpu.VMEM((2, c), F32),
    ] + [pltpu.VMEM((1, c), F32)] * 4 + [
        pltpu.VMEM((c, 4 * c), BF16), pltpu.VMEM((c, c), BF16), pltpu.VMEM((c, c), BF16),
        pltpu.VMEM((c, 4 * c), BF16), pltpu.VMEM((c, c), BF16), pltpu.VMEM((c, c), BF16),
        pltpu.VMEM((c, 8), F32), pltpu.VMEM((2, total), F32), pltpu.VMEM((4 * c, total), BF16), full(F32), full(BF16), full(F32),
        pltpu.VMEM((4 * c, total), F32), full(F32), full(BF16), full(F32), full(BF16), full(F32), full(BF16),
        block(parts, m, hs), block(parts, m, hs), block(parts, m, hs),
        block(parts, m, hs), block(parts, n, hs), block(parts, m, hs),
        block(2, m, wh), block(2, m, wh), block(n, wh), block(n, wh),
        block(m, wh), block(n, wh), block(2, m, wh), block(2, m, wh),
        block(2, small, we), block(2, small, we), block(small, we), block(small, we),
        block(small, we), block(small, we), block(2, small, we), block(2, small, we),
        slab, slab, slab,
        pltpu.VMEM((wh, m * rows, res), BF16), pltpu.VMEM((wh, m * rows, res), BF16),
        pltpu.VMEM((we, res, res), BF16), pltpu.VMEM((we, res, res), BF16),
        pltpu.VMEM((groups, c, wide), F32), pltpu.VMEM((c, c), F32), pltpu.VMEM((c, c), F32),
        pltpu.VMEM((c, 1), F32), pltpu.VMEM((c, 1), F32),
        pltpu.VMEM((m, hc, wide), BF16), pltpu.VMEM((n, hc, wide), BF16),
        pltpu.VMEM((hc, wide), BF16), pltpu.VMEM((m, hc, wide), BF16),
    ] + [
        pltpu.VMEM(shape, BF16)
        for shape in ((m, hc, 2 * c), (m, hc, 2 * c), (hc, 2 * c), (hc, 2 * c), (hc, 2 * c), (m, hc, 2 * c))
    ] + [
        pltpu.VMEM(shape, BF16) for shape in ((m, hc, wide), (n, hc, wide), (hc, wide), (m, hc, wide))
    ] + [
        pltpu.VMEM((2, c), F32), pltpu.VMEM((n, 2, c), F32),
        pltpu.SemaphoreType.DMA((15,)), pltpu.SemaphoreType.DMA((17,)), pltpu.SemaphoreType.DMA((receive_slots(parts, chunks)[-1],)),
    ]
    vmem = pl.BlockSpec(memory_space=pltpu.VMEM)
    results = pl.pallas_call(
        functools.partial(kernel, n, rows, res, lc, pitch, every),
        out_shape=(
            pltpu.VMEM((total, c), BF16),
            pltpu.VMEM((c, 4 * c), F32),
            pltpu.VMEM((c, c), F32),
            pltpu.VMEM((c, c), F32),
            pltpu.VMEM((1, c), F32),
            pltpu.VMEM((1, c), F32),
        ),
        in_specs=[pl.BlockSpec(memory_space=pl.ANY)] * 15,
        out_specs=(vmem,) * 6,
        scratch_shapes=scratch,
        compiler_params=pltpu.CompilerParams(
            collective_id=0, has_side_effects=True, vmem_limit_bytes=56 * 1024 * 1024
        ),
    )(
        pair.reshape(total, c), cotangent.reshape(total, c),
        residue_mask.reshape(1, res), chain_ids.reshape(1, res), chain_embed,
        out_norm_gain.reshape(1, c), out_mid_gain.reshape(1, c),
        in_norm_gain.reshape(1, c), in_mid_gain.reshape(1, c),
        out_proj, out_gate, out_final, in_proj, in_gate, in_final,
    )
    shapes = [((total, c), BF16), ((c, 4 * c), F32), ((c, c), F32), ((c, c), F32), ((1, c), F32), ((1, c), F32)]
    grad, gp, gg, gf, gn, gm = pl.pallas_call(
        write_out,
        out_shape=[jax.ShapeDtypeStruct(*shape) for shape in shapes],
        in_specs=[pl.BlockSpec(memory_space=pltpu.VMEM)] * 6,
        out_specs=[pl.BlockSpec(memory_space=pl.ANY)] * 6,
        scratch_shapes=[pltpu.SemaphoreType.DMA((6,))],
    )(*[pltpu.with_memory_space_constraint(r, pltpu.VMEM) for r in results])
    return grad.reshape(rows, res, c), gp, gg, gf, gn.reshape(c), gm.reshape(c)


def solution(mesh):
    split = P("dap", "cplx", None)
    return jax.shard_map(
        functools.partial(shards, mesh.shape["dap"]),
        mesh=mesh,
        in_specs=(split, split, P("cplx"), P("cplx")) + (P(),) * 11,
        out_specs=(split, P("cplx", None), P("cplx", None), P("cplx", None), P("cplx"), P("cplx")),
        check_vma=False,
    )
```
